32 devices in a mesh: dp: 1 (over z), sp: 32 (over y, x, core).
Axes of the slice: x: 4, y: 4, z: 1, core: 2. Of those that a mesh axis runs over, the one named last changes fastest.
The devices are a block of a 4x4x8 slice.
Arguments:
- tokens: bfloat16 [64, 5120], P('dp')
- positions: int32 [64], P('dp')
- k_cache: bfloat16 [64, 2048, 8, 128], P('dp', 'sp')
- v_cache: bfloat16 [64, 2048, 8, 128], P('dp', 'sp')
- w_q: bfloat16 [5120, 5120], replicated
- w_k: bfloat16 [5120, 1024], replicated
- w_v: bfloat16 [5120, 1024], replicated
- w_o: bfloat16 [5120, 5120], replicated
- attn_norm: bfloat16 [5120], replicated
- q_norm: bfloat16 [128], replicated
- k_norm: bfloat16 [128], replicated
Outputs:
- output 1: bfloat16 [64, 5120], P('dp')
- output 2: bfloat16 [64, 2048, 8, 128], P('dp', 'sp')
- output 3: bfloat16 [64, 2048, 8, 128], P('dp', 'sp')
- output 4: bfloat16 [64, 2, 8, 128], P('dp')
All inputs are finite; a program needn't handle non-finite values.
Results may differ from the reference program's by a relative error of at most 0.00657234.
Values sent between devices are 32-bit elements.
A program may use at most 768 MiB of HBM per device.

```python
import jax
import jax.numpy as jnp
from jax import lax

NUM_SEQS = 64
MODEL_DIM = 5120
Q_HEADS = 40
KV_HEADS = 8
HEAD_DIM = 128
CACHE_LEN = 2048

Q_PER_KV = Q_HEADS // KV_HEADS
NORM_EPS = 1e-6
ROPE_THETA = 1000000.0
NEG_FILL = -1e30


def setup_inputs(seed: int = 0, part: int = 0) -> dict:
    part_keys = jax.random.split(jax.random.fold_in(jax.random.key(seed), part), 5)
    shared = jax.random.split(jax.random.key(seed + 1), 7)
    cache_shape = (NUM_SEQS, CACHE_LEN, KV_HEADS, HEAD_DIM)
    tokens = jax.random.normal(part_keys[0], (NUM_SEQS, MODEL_DIM), jnp.float32)
    pos_draw = jax.random.randint(part_keys[1], (NUM_SEQS,), CACHE_LEN // 4, CACHE_LEN, dtype=jnp.int32)
    positions = pos_draw.at[0].set(CACHE_LEN - 1).at[1].set(CACHE_LEN // 4)
    k_cache = jax.random.normal(part_keys[2], cache_shape, jnp.float32)
    coarse = jax.random.normal(part_keys[3], (NUM_SEQS, 16, KV_HEADS, HEAD_DIM), jnp.float32)
    v_noise = jax.random.normal(part_keys[4], cache_shape, jnp.float32)
    v_cache = 1.5 * jnp.repeat(coarse, CACHE_LEN // 16, axis=1) + 0.5 * v_noise
    w_q = jax.random.normal(shared[0], (MODEL_DIM, Q_HEADS * HEAD_DIM), jnp.float32) * MODEL_DIM ** -0.5
    w_k = jax.random.normal(shared[1], (MODEL_DIM, KV_HEADS * HEAD_DIM), jnp.float32) * MODEL_DIM ** -0.5
    w_v = jax.random.normal(shared[2], (MODEL_DIM, KV_HEADS * HEAD_DIM), jnp.float32) * MODEL_DIM ** -0.5
    w_o = jax.random.normal(shared[3], (Q_HEADS * HEAD_DIM, MODEL_DIM), jnp.float32) * (Q_HEADS * HEAD_DIM) ** -0.5
    attn_norm = jax.random.uniform(shared[4], (MODEL_DIM,), jnp.float32, 0.5, 1.5)
    q_norm = jax.random.uniform(shared[5], (HEAD_DIM,), jnp.float32, 0.5, 2.0)
    k_norm = jax.random.uniform(shared[6], (HEAD_DIM,), jnp.float32, 0.5, 2.0)
    return {
        'tokens': tokens.astype(jnp.bfloat16),
        'positions': positions,
        'k_cache': k_cache.astype(jnp.bfloat16),
        'v_cache': v_cache.astype(jnp.bfloat16),
        'w_q': w_q.astype(jnp.bfloat16),
        'w_k': w_k.astype(jnp.bfloat16),
        'w_v': w_v.astype(jnp.bfloat16),
        'w_o': w_o.astype(jnp.bfloat16),
        'attn_norm': attn_norm.astype(jnp.bfloat16),
        'q_norm': q_norm.astype(jnp.bfloat16),
        'k_norm': k_norm.astype(jnp.bfloat16),
    }


def rms_scale(values, gain):
    return values * lax.rsqrt(jnp.mean(values * values, axis=-1, keepdims=True) + NORM_EPS) * gain.astype(jnp.float32)


def rope_table(positions):
    inv_freq = ROPE_THETA ** (-jnp.arange(HEAD_DIM // 2, dtype=jnp.float32) * 2.0 / HEAD_DIM)
    angles = positions.astype(jnp.float32)[:, None] * inv_freq[None, :]
    return jnp.cos(angles)[:, None, :], jnp.sin(angles)[:, None, :]


def norm_rope(proj, gain, cos_table, sin_table):
    normed = rms_scale(proj.astype(jnp.float32), gain)
    first_half = normed[..., :HEAD_DIM // 2]
    second_half = normed[..., HEAD_DIM // 2:]
    rotated = jnp.concatenate([first_half * cos_table - second_half * sin_table, second_half * cos_table + first_half * sin_table], axis=-1)
    return rotated.astype(jnp.bfloat16)


def reference(tokens, positions, k_cache, v_cache, w_q, w_k, w_v, w_o, attn_norm, q_norm, k_norm):
    tokens_f = tokens.astype(jnp.float32)
    hidden = rms_scale(tokens_f, attn_norm).astype(jnp.bfloat16)
    q_proj = jnp.dot(hidden, w_q, preferred_element_type=jnp.float32).astype(jnp.bfloat16).reshape(NUM_SEQS, Q_HEADS, HEAD_DIM)
    k_proj = jnp.dot(hidden, w_k, preferred_element_type=jnp.float32).astype(jnp.bfloat16).reshape(NUM_SEQS, KV_HEADS, HEAD_DIM)
    v_new = jnp.dot(hidden, w_v, preferred_element_type=jnp.float32).astype(jnp.bfloat16).reshape(NUM_SEQS, KV_HEADS, HEAD_DIM)
    cos_table, sin_table = rope_table(positions)
    q_rot = norm_rope(q_proj, q_norm, cos_table, sin_table)
    k_rot = norm_rope(k_proj, k_norm, cos_table, sin_table)
    slot_ids = jnp.arange(CACHE_LEN)
    write_mask = (slot_ids[None, :] == positions[:, None])[:, :, None, None]
    k_out = jnp.where(write_mask, k_rot[:, None], k_cache)
    v_out = jnp.where(write_mask, v_new[:, None], v_cache)
    score_scale = HEAD_DIM ** -0.5

    def one_seq(items):
        q_one, k_one, v_one, pos_one = items
        q_grp = q_one.reshape(KV_HEADS, Q_PER_KV, HEAD_DIM).astype(jnp.float32)
        scores = jnp.einsum('kgd,tkd->kgt', q_grp, k_one.astype(jnp.float32)) * score_scale
        live_mask = (slot_ids <= pos_one)[None, None, :]
        global_peak = jnp.max(jnp.where(live_mask, scores, NEG_FILL), axis=-1, keepdims=True)
        weights = jnp.where(live_mask, jnp.exp(scores - global_peak), 0.0)
        total_sum = jnp.sum(weights, axis=-1, keepdims=True)
        mixed = jnp.einsum('kgt,tkd->kgd', weights.astype(jnp.bfloat16).astype(jnp.float32), v_one.astype(jnp.float32))
        return (mixed / total_sum).astype(jnp.bfloat16).reshape(Q_HEADS * HEAD_DIM)

    attn_out = lax.map(one_seq, (q_rot, k_out, v_out, positions))
    block_out = (tokens_f + jnp.dot(attn_out, w_o, preferred_element_type=jnp.float32)).astype(jnp.bfloat16)
    new_kv = jnp.stack([k_rot, v_new], axis=1)
    return (block_out, k_out, v_out, new_kv)
```

```python
import functools

import jax
import jax.numpy as jnp
from jax import lax
from jax.experimental import pallas as pl
from jax.experimental.pallas import tpu as pltpu
from jax.sharding import PartitionSpec as P

NORM_EPS = 1e-6
ROPE_THETA = 1000000.0
NEG_FILL = -1e30
MESH = pl.DeviceIdType.MESH
F32 = jnp.float32
BF16 = jnp.bfloat16


def rms_scale(values, gain):
    return values * lax.rsqrt(jnp.mean(values * values, axis=-1, keepdims=True) + NORM_EPS) * gain.astype(F32)


def rope_table(positions, head_dim):
    inv_freq = ROPE_THETA ** (-jnp.arange(head_dim // 2, dtype=F32) * 2.0 / head_dim)
    angles = positions.astype(F32)[:, None] * inv_freq[None, :]
    return jnp.cos(angles)[:, None, :], jnp.sin(angles)[:, None, :]


def norm_rope(proj, gain, cos_table, sin_table):
    normed = rms_scale(proj.astype(F32), gain)
    half_dim = proj.shape[-1] // 2
    first_half = normed[..., :half_dim]
    second_half = normed[..., half_dim:]
    rotated = jnp.concatenate([first_half * cos_table - second_half * sin_table, second_half * cos_table + first_half * sin_table], axis=-1)
    return rotated.astype(BF16)


def project_token(tokens, positions, w_q, w_k, w_v, attn_norm, q_norm, k_norm):
    seq_count = tokens.shape[0]
    head_dim = q_norm.shape[0]
    hidden = rms_scale(tokens.astype(F32), attn_norm).astype(BF16)
    q_proj = jnp.dot(hidden, w_q, preferred_element_type=F32).astype(BF16).reshape(seq_count, -1, head_dim)
    k_proj = jnp.dot(hidden, w_k, preferred_element_type=F32).astype(BF16).reshape(seq_count, -1, head_dim)
    v_new = jnp.dot(hidden, w_v, preferred_element_type=F32).astype(BF16).reshape(seq_count, -1, head_dim)
    cos_table, sin_table = rope_table(positions, head_dim)
    return norm_rope(q_proj, q_norm, cos_table, sin_table), norm_rope(k_proj, k_norm, cos_table, sin_table), v_new


def attn_body(seqs, slots, kv_heads, q_heads, pos_ref, start_ref, q_ref, kv_ref, k_ref, v_ref, ko_ref, vo_ref, o_ref, ml_ref):
    head_dim = q_ref.shape[-1]
    step = pl.program_id(0)
    scale = head_dim ** -0.5
    cols = slots * kv_heads
    group = q_heads // kv_heads
    row_id = lax.broadcasted_iota(jnp.int32, (q_heads, cols), 0)
    col_id = lax.broadcasted_iota(jnp.int32, (q_heads, cols), 1)
    own_head = jnp.zeros((q_heads, cols), jnp.int32)
    for h in range(1, kv_heads):
        own_head += (row_id >= h * group).astype(jnp.int32)
    slot_of = jnp.where(lax.rem(col_id, kv_heads) == own_head, lax.div(col_id, kv_heads), 1 << 20)
    upper = lax.broadcasted_iota(jnp.int32, (2 * kv_heads, head_dim), 0) >= kv_heads
    diag_r = lax.broadcasted_iota(jnp.int32, (q_heads, head_dim), 0)
    diag_c = lax.broadcasted_iota(jnp.int32, (q_heads, head_dim), 1)
    diag = diag_r == diag_c
    for b in range(seqs):
        rel = pos_ref[step * seqs + b] - start_ref[0]
        ko_ref[b] = k_ref[b]
        vo_ref[b] = v_ref[b]

        @pl.when((rel >= 0) & (rel < slots))
        def _():
            tile = lax.div(rel, 2)
            hit = upper == (lax.rem(rel, 2) == 1)
            k_new = kv_ref[pl.ds(b * 2 * kv_heads, kv_heads), :]
            v_new = kv_ref[pl.ds(b * 2 * kv_heads + kv_heads, kv_heads), :]
            k_two = jnp.concatenate([k_new, k_new], axis=0)
            v_two = jnp.concatenate([v_new, v_new], axis=0)
            ko_ref[b, tile] = jnp.where(hit, k_two, ko_ref[b, tile].astype(F32)).astype(BF16)
            vo_ref[b, tile] = jnp.where(hit, v_two, vo_ref[b, tile].astype(F32)).astype(BF16)

    for b in range(seqs):
        rel = pos_ref[step * seqs + b] - start_ref[0]
        keys = ko_ref[b].reshape(cols, head_dim)
        vals = vo_ref[b].reshape(cols, head_dim)
        query = q_ref[pl.ds(b * q_heads, q_heads), :].astype(BF16)
        scores = lax.dot_general(query, keys, (((1,), (1,)), ((), ())), preferred_element_type=F32) * scale
        live = slot_of <= rel
        scores = jnp.where(live, scores, NEG_FILL)
        peak = jnp.max(scores, axis=1, keepdims=True)
        weights = jnp.where(live, jnp.exp(scores - peak), 0.0)
        total = jnp.sum(weights, axis=1, keepdims=True)
        o_ref[pl.ds(b * q_heads, q_heads), :] = jnp.dot(weights.astype(BF16), vals, preferred_element_type=F32)
        ml_ref[0, 0, pl.ds(b, 1), :] = jnp.sum(jnp.where(diag, peak, 0.0), axis=0, keepdims=True)
        ml_ref[0, 1, pl.ds(b, 1), :] = jnp.sum(jnp.where(diag, total, 0.0), axis=0, keepdims=True)


def attention(q_rows, kv_rows, positions, shard_start, k_cache, v_cache):
    seq_count, slots, kv_heads, head_dim = k_cache.shape
    q_heads = q_rows.shape[0] // seq_count
    seqs = 8
    steps = seq_count // seqs
    pairs = slots // 2
    k4 = k_cache.reshape(seq_count, pairs, 2 * kv_heads, head_dim)
    v4 = v_cache.reshape(seq_count, pairs, 2 * kv_heads, head_dim)
    cache_block = pl.BlockSpec((seqs, pairs, 2 * kv_heads, head_dim), lambda i, *_: (i, 0, 0, 0))
    grid_spec = pltpu.PrefetchScalarGridSpec(
        num_scalar_prefetch=2,
        grid=(steps,),
        in_specs=[
            pl.BlockSpec((seqs * q_heads, head_dim), lambda i, *_: (i, 0)),
            pl.BlockSpec((seqs * 2 * kv_heads, head_dim), lambda i, *_: (i, 0)),
            cache_block,
            cache_block,
        ],
        out_specs=[
            cache_block,
            cache_block,
            pl.BlockSpec((seqs * q_heads, head_dim), lambda i, *_: (i, 0)),
            pl.BlockSpec((1, 2, seqs, head_dim), lambda i, *_: (i, 0, 0, 0)),
        ],
    )
    k_out, v_out, part, ml = pl.pallas_call(
        functools.partial(attn_body, seqs, slots, kv_heads, q_heads),
        grid_spec=grid_spec,
        out_shape=[
            jax.ShapeDtypeStruct(k4.shape, BF16),
            jax.ShapeDtypeStruct(v4.shape, BF16),
            jax.ShapeDtypeStruct((seq_count * q_heads, head_dim), F32),
            jax.ShapeDtypeStruct((steps, 2, seqs, head_dim), F32),
        ],
        compiler_params=pltpu.CompilerParams(dimension_semantics=("arbitrary",)),
        name="attend",
    )(positions, shard_start, q_rows, kv_rows, k4, v4)
    return k_out.reshape(k_cache.shape), v_out.reshape(v_cache.shape), part, ml


def blend(parts, stats, seqs, q_heads, row0=0):
    peak = stats[0][0]
    for m, _ in stats[1:]:
        peak = jnp.maximum(peak, m)
    factors = [jnp.exp(m - peak) for m, _ in stats]
    total = factors[0] * stats[0][1]
    for f, (_, l) in zip(factors[1:], stats[1:]):
        total += f * l
    return peak, total, factors


def columns_of(tile):
    return jnp.transpose(tile)


def combine_body(side, q_heads, o_ref, ml_ref, tok_ref, wo_ref, out_ref,
                 r1, rm1, s1, sm1, r2, rm2, s2, sm2, r3, rm3, obuf, lhs, wbuf, gbuf, acc,
                 w_sem, a_s, a_r, b_s, b_r, c_s, c_r, d_s, d_r, e_s, e_r, f_s, f_r, h_s, h_r):
    me = lax.axis_index("sp")
    core = lax.rem(me, 2)
    chip = lax.div(me, 2)
    x = lax.rem(chip, side)
    y = lax.div(chip, side)
    first = x * (1 - core) + y * core
    second = y * (1 - core) + x * core
    stride1 = 2 * (1 - core) + 2 * side * core
    stride2 = 2 * side * (1 - core) + 2 * core
    partner = me + 1 - 2 * core
    head_dim = o_ref.shape[-1]
    width = wbuf.shape[1]
    depth = wbuf.shape[0]
    w_parts = w_sem.shape[0]
    w_rows = depth // w_parts
    order = [side // 2] + [d for d in range(1, side) if d != side // 2]

    def peer1(d):
        return me + (lax.rem(first + d, side) - first) * stride1

    def peer2(d):
        return me + (lax.rem(second + d, side) - second) * stride2

    def send(src, dst, ssem, rsem, to):
        copy = pltpu.make_async_remote_copy(src_ref=src, dst_ref=dst, send_sem=ssem, recv_sem=rsem, device_id={"sp": to}, device_id_type=MESH)
        copy.start()
        return copy

    w_copies = []
    for i in range(w_parts):
        copy = pltpu.make_async_copy(
            wo_ref.at[pl.ds(i * w_rows, w_rows), pl.ds(pl.multiple_of(core * width, 128), width)],
            wbuf.at[pl.ds(i * w_rows, w_rows), :], w_sem.at[i])
        copy.start()
        w_copies.append(copy)

    barrier = pltpu.get_barrier_semaphore()
    neighbours = [partner] + [peer1(d) for d in range(1, side)] + [peer2(d) for d in range(1, side)]
    for n in neighbours:
        pl.semaphore_signal(barrier, inc=1, device_id={"sp": n}, device_id_type=MESH)
    pl.semaphore_wait(barrier, len(neighbours))

    started = []
    in1 = {}
    for d in order + [0]:
        piece = lax.rem(second + d, side)
        in1[d] = (send(o_ref.at[1 - core, piece], r1.at[d], a_s.at[d, 0], a_r.at[d, 0], partner),
                  send(ml_ref.at[1 - core, piece], rm1.at[d], a_s.at[d, 1], a_r.at[d, 1], partner))
    in2 = {}
    for d in order + [0]:
        in1[d][0].wait_recv()
        in1[d][1].wait_recv()
        piece = lax.rem(first + d, side)
        own_m, own_l = ml_ref[core, piece, 0], ml_ref[core, piece, 1]
        peak, total, fac = blend(None, [(own_m, own_l), (rm1[d, 0], rm1[d, 1])], None, None)
        sm1[d, 0] = peak
        sm1[d, 1] = total
        cols = [columns_of(f) for f in fac]
        for k in range(side):
            for i in range(2):
                seq = 2 * k + i
                rows = pl.ds(i * q_heads, q_heads)
                s1[d, k, rows, :] = (o_ref[core, piece, k, rows, :] * cols[0][:q_heads, seq:seq + 1]
                                     + r1[d, k, rows, :] * cols[1][:q_heads, seq:seq + 1])
        if d:
            in2[d] = (send(s1.at[d], r2.at[d], b_s.at[d, 0], b_r.at[d, 0], peer1(d)),
                      send(sm1.at[d], rm2.at[d], b_s.at[d, 1], b_r.at[d, 1], peer1(d)))
    for d in order:
        in2[d][0].wait_recv()
        in2[d][1].wait_recv()
    stats = [(sm1[0, 0], sm1[0, 1])] + [(rm2[d, 0], rm2[d, 1]) for d in range(1, side)]
    peak, total, fac = blend(None, stats, None, None)
    sm2[0] = peak
    sm2[1] = total
    cols = [columns_of(f) for f in fac]
    for k in range(side):
        for i in range(2):
            seq = 2 * k + i
            rows = pl.ds(i * q_heads, q_heads)
            value = s1[0, k, rows, :] * cols[0][:q_heads, seq:seq + 1]
            for d in range(1, side):
                value += r2[d, k, rows, :] * cols[d][:q_heads, seq:seq + 1]
            s2[k, rows, :] = value
    in3 = {}
    for d in order:
        in3[d] = (send(s2.at[lax.rem(second + d, side)], r3.at[d], c_s.at[d, 0], c_r.at[d, 0], peer2(d)),
                  send(sm2, rm3.at[d], c_s.at[d, 1], c_r.at[d, 1], peer2(d)))
    for d in order:
        in3[d][0].wait_recv()
        in3[d][1].wait_recv()
    stats = [(sm2[0], sm2[1])] + [(rm3[d, 0], rm3[d, 1]) for d in range(1, side)]
    peak, total, fac = blend(None, stats, None, None)
    rm3[0, 0] = total
    for d in range(side):
        rm3[d, 1] = fac[d]
    mine = pl.ds(2 * second, 2)
    cols = []
    for d in range(side):
        cols.append(columns_of(jnp.concatenate([rm3[d, 1, mine, :]] * 4, axis=0)))
    l_cols = columns_of(jnp.concatenate([rm3[0, 0, mine, :]] * 4, axis=0))
    for i in range(2):
        rows = pl.ds(i * q_heads, q_heads)
        value = s2[second, rows, :] * cols[0][:q_heads, i:i + 1]
        for d in range(1, side):
            value += r3[d, rows, :] * cols[d][:q_heads, i:i + 1]
        value = value / l_cols[:q_heads, i:i + 1]
        obuf[core, rows, :] = value.astype(BF16).astype(F32)
    swap = send(obuf.at[core], obuf.at[core], d_s, d_r, partner)
    swap.wait_recv()

    for i in range(2):
        for h in range(q_heads):
            lhs[i:i + 1, h * head_dim:(h + 1) * head_dim] = obuf[0, i * q_heads + h:i * q_heads + h + 1, :]
            lhs[2 + i:3 + i, h * head_dim:(h + 1) * head_dim] = obuf[1, i * q_heads + h:i * q_heads + h + 1, :]
    for copy in w_copies:
        copy.wait()
    left = lhs[...].astype(BF16)

    def pair_a(f, s):
        return (f * side + s) * (1 - core) + (s * side + f) * core

    def pair_b(f, s):
        return side * side + (s * side + f) * (1 - core) + (f * side + s) * core

    pa, pb = pair_a(first, second), pair_b(first, second)
    n_step = 512
    for n in range(0, width, n_step):
        prod = jnp.dot(left, wbuf[:, n:n + n_step], preferred_element_type=F32)
        gbuf[core, pa, :, n:n + n_step] = prod[0:2]
        gbuf[core, pb, :, n:n + n_step] = prod[2:4]

    g1, g2, g3 = {}, {}, {}
    for d in order:
        for ab, p in enumerate((pa, pb)):
            g1[d, ab] = send(gbuf.at[core, p], gbuf.at[core, p], e_s.at[d, ab], e_r.at[d, ab], peer1(d))
    for ab, p in enumerate((pa, pb)):
        for e in order:
            g2[e, 0, ab] = send(gbuf.at[core, p], gbuf.at[core, p], f_s.at[e, 0, ab], f_r.at[e, 0, ab], peer2(e))
        g3[0, 0, ab] = send(gbuf.at[core, p], gbuf.at[core, p], h_s.at[0, 0, ab], h_r.at[0, 0, ab], partner)
    for d in order:
        f_from = lax.rem(first - d + side, side)
        for ab, p in enumerate((pair_a(f_from, second), pair_b(f_from, second))):
            g1[d, ab].wait_recv()
            for e in order:
                g2[e, d, ab] = send(gbuf.at[core, p], gbuf.at[core, p], f_s.at[e, d, ab], f_r.at[e, d, ab], peer2(e))
            g3[0, d, ab] = send(gbuf.at[core, p], gbuf.at[core, p], h_s.at[0, d, ab], h_r.at[0, d, ab], partner)
    for d in [0] + order:
        f_from = lax.rem(first - d + side, side)
        for e in order:
            s_from = lax.rem(second - e + side, side)
            for ab, p in enumerate((pair_a(f_from, s_from), pair_b(f_from, s_from))):
                g2[e, d, ab].wait_recv()
                g3[e, d, ab] = send(gbuf.at[core, p], gbuf.at[core, p], h_s.at[e, d, ab], h_r.at[e, d, ab], partner)
    for key in g3:
        g3[key].wait_recv()
    for half in range(2):
        for p in range(2 * side * side):
            acc[2 * p:2 * p + 2, half * width:(half + 1) * width] = gbuf[half, p]
    out_ref[...] = (tok_ref[...].astype(F32) + acc[...]).astype(BF16)

    for group in (in1, in2, in3):
        for pair in group.values():
            pair[0].wait_send()
            pair[1].wait_send()
    swap.wait_send()
    for group in (g1, g2, g3):
        for copy in group.values():
            copy.wait_send()


def combine(part, ml, tokens, w_o, side):
    seq_count, dim = tokens.shape
    head_dim = part.shape[-1]
    q_heads = part.shape[0] // seq_count
    rows = 2 * q_heads
    o5 = part.reshape(2, side, side, rows, head_dim)
    m5 = ml.reshape(2, side, 2, ml.shape[2], head_dim)
    width = dim // 2
    depth = w_o.shape[0]
    dma = pltpu.SemaphoreType.DMA
    vmem = pl.BlockSpec(memory_space=pltpu.VMEM)
    piece = (side, side, rows, head_dim)
    stat = (side, 2, ml.shape[2], head_dim)
    return pl.pallas_call(
        functools.partial(combine_body, side, q_heads),
        out_shape=jax.ShapeDtypeStruct(tokens.shape, BF16),
        in_specs=[vmem, vmem, vmem, pl.BlockSpec(memory_space=pl.ANY)],
        out_specs=vmem,
        scratch_shapes=[
            pltpu.VMEM(piece, F32), pltpu.VMEM(stat, F32),
            pltpu.VMEM(piece, F32), pltpu.VMEM(stat, F32),
            pltpu.VMEM(piece, F32), pltpu.VMEM(stat, F32),
            pltpu.VMEM(piece[1:], F32), pltpu.VMEM(stat[1:], F32),
            pltpu.VMEM(piece[1:], F32), pltpu.VMEM(stat, F32),
            pltpu.VMEM((2, rows, head_dim), F32),
            pltpu.VMEM((8, depth), F32),
            pltpu.VMEM((depth, width), BF16),
            pltpu.VMEM((2, 2 * side * side, 2, width), F32),
            pltpu.VMEM(tokens.shape, F32),
            dma((4,)),
            dma((side, 2)), dma((side, 2)),
            dma((side, 2)), dma((side, 2)),
            dma((side, 2)), dma((side, 2)),
            dma, dma,
            dma((side, 2)), dma((side, 2)),
            dma((side, side, 2)), dma((side, side, 2)),
            dma((side, side, 2)), dma((side, side, 2)),
        ],
        compiler_params=pltpu.CompilerParams(collective_id=1, has_side_effects=True, vmem_limit_bytes=60 * 1024 * 1024),
        name="combine",
    )(o5, m5, tokens, w_o)


def solution(mesh):
    cache_spec = P('dp', 'sp', None, None)
    side = int(round((mesh.shape['sp'] // 2) ** 0.5))

    def device_step(tokens, positions, k_cache, v_cache, w_q, w_k, w_v, w_o, attn_norm, q_norm, k_norm):
        q_rot, k_rot, v_new = project_token(tokens, positions, w_q, w_k, w_v, attn_norm, q_norm, k_norm)
        head_dim = q_norm.shape[0]
        new_kv = jnp.stack([k_rot, v_new], axis=1)
        shard_start = (lax.axis_index('sp') * k_cache.shape[1]).astype(jnp.int32).reshape(1)
        q_rows = q_rot.astype(F32).reshape(-1, head_dim)
        kv_rows = new_kv.astype(F32).reshape(-1, head_dim)
        k_upd, v_upd, part, ml = attention(q_rows, kv_rows, positions, shard_start, k_cache, v_cache)
        block_out = combine(part, ml, tokens, w_o, side)
        return block_out, k_upd, v_upd, new_kv

    return jax.shard_map(device_step, mesh=mesh, in_specs=(P('dp', None), P('dp'), cache_spec, cache_spec, P(), P(), P(), P(), P(), P(), P()), out_specs=(P('dp', None), cache_spec, cache_spec, P('dp', None, None, None)), check_vma=False)
```

```python
import functools

import jax
import jax.numpy as jnp
import numpy as np
from jax import lax
from jax.experimental import pallas as pl
from jax.experimental.pallas import tpu as pltpu
from jax.sharding import PartitionSpec as P

NORM_EPS = 1e-6
ROPE_THETA = 1000000.0
NEG_FILL = -1e30
MESH = pl.DeviceIdType.MESH
F32 = jnp.float32
BF16 = jnp.bfloat16


def project_body(seq_count, q_heads, kv_heads, head_dim, tok_ref, gain_ref, pos_ref, freq_ref, wq_ref, wk_ref, wv_ref,
                 q_ref, kv_ref, hid, wbuf, stage, taken, w_sem, s_sem, r_sem):
    me = lax.axis_index("sp")
    core = lax.rem(me, 2)
    partner = me + 1 - 2 * core
    dim = tok_ref.shape[1]
    chunks, _, width = wbuf.shape
    per = width // head_dim
    splits = w_sem.shape[1]
    rows = dim // splits
    kv_chunks = kv_heads // 2 // per
    q_chunks = chunks - 2 * kv_chunks

    def source(i):
        if i < kv_chunks:
            return wk_ref, core * (kv_heads // 2) + i * per
        if i < 2 * kv_chunks:
            return wv_ref, core * (kv_heads // 2) + (i - kv_chunks) * per
        return wq_ref, core * (q_heads // 2) + (i - 2 * kv_chunks) * per

    def fetch(i, j):
        ref, head = source(i)
        return pltpu.make_async_copy(
            ref.at[pl.ds(j * rows, rows), pl.ds(pl.multiple_of(head * head_dim, 128), width)],
            wbuf.at[i, pl.ds(j * rows, rows), :], w_sem.at[i, j])

    pieces = [(i, j) for i in range(chunks) for j in range(splits)]
    ahead = 5
    for i, j in pieces[:ahead]:
        fetch(i, j).start()

    barrier = pltpu.get_barrier_semaphore()
    pl.semaphore_signal(barrier, inc=1, device_id={"sp": partner}, device_id_type=MESH)

    gain = gain_ref[:, :dim]
    q_gain = gain_ref[:, dim:dim + head_dim]
    k_gain = gain_ref[:, dim + head_dim:dim + 2 * head_dim]
    tok = tok_ref[...].astype(F32)
    hid[...] = (tok * lax.rsqrt(jnp.mean(tok * tok, axis=-1, keepdims=True) + NORM_EPS) * gain).astype(BF16)
    eye = lax.broadcasted_iota(jnp.int32, (seq_count, seq_count), 0) == lax.broadcasted_iota(jnp.int32, (seq_count, seq_count), 1)
    pos = jnp.sum(jnp.where(eye, pos_ref[...].astype(F32), 0.0), axis=1, keepdims=True)
    angles = pos * freq_ref[...]
    cos = jnp.cos(angles)
    lower = lax.broadcasted_iota(jnp.int32, (seq_count, head_dim), 1) < head_dim // 2
    sin = jnp.sin(angles)
    sin = jnp.where(lower, -sin, sin)
    pl.semaphore_wait(barrier, 1)

    def place(i, side, buf):
        for n in range(per):
            value = buf[i, :, n * head_dim:(n + 1) * head_dim]
            if i < 2 * kv_chunks:
                head = side * (kv_heads // 2) + (i % kv_chunks) * per + n + (kv_heads if i >= kv_chunks else 0)
                kv_ref[pl.ds(head, seq_count, stride=2 * kv_heads), :] = value
            else:
                head = side * (q_heads // 2) + (i - 2 * kv_chunks) * per + n
                q_ref[pl.ds(head, seq_count, stride=q_heads), :] = value

    swaps = []
    for i in range(chunks):
        acc = None
        for j in range(splits):
            at = i * splits + j
            fetch(i, j).wait()
            if at + ahead < len(pieces):
                fetch(*pieces[at + ahead]).start()
            part = jnp.dot(hid[:, j * rows:(j + 1) * rows], wbuf[i, j * rows:(j + 1) * rows, :], preferred_element_type=F32)
            acc = part if acc is None else acc + part
        acc = acc.astype(BF16).astype(F32)
        for n in range(per):
            value = acc[:, n * head_dim:(n + 1) * head_dim]
            if not kv_chunks <= i < 2 * kv_chunks:
                scale = lax.rsqrt(jnp.mean(value * value, axis=-1, keepdims=True) + NORM_EPS)
                value = value * scale * (k_gain if i < kv_chunks else q_gain)
                value = value * cos + pltpu.roll(value, head_dim // 2, 1) * sin
                value = value.astype(BF16).astype(F32)
            stage[i, :, n * head_dim:(n + 1) * head_dim] = value
        copy = pltpu.make_async_remote_copy(
            src_ref=stage.at[i], dst_ref=taken.at[i], send_sem=s_sem.at[i], recv_sem=r_sem.at[i],
            device_id={"sp": partner}, device_id_type=MESH)
        copy.start()
        swaps.append(copy)
        place(i, core, stage)
        if i > 0:
            swaps[i - 1].wait_recv()
            place(i - 1, 1 - core, taken)
    swaps[-1].wait_recv()
    place(chunks - 1, 1 - core, taken)
    for copy in swaps:
        copy.wait_send()


def project(tokens, positions, w_q, w_k, w_v, attn_norm, q_norm, k_norm):
    seq_count, dim = tokens.shape
    head_dim = q_norm.shape[0]
    q_heads = w_q.shape[1] // head_dim
    kv_heads = w_k.shape[1] // head_dim
    width = 4 * head_dim
    chunks = (w_q.shape[1] + w_k.shape[1] + w_v.shape[1]) // 2 // width
    splits = 2
    gains = jnp.concatenate([attn_norm, q_norm, k_norm]).astype(F32).reshape(1, -1)
    half = ROPE_THETA ** (-np.arange(head_dim // 2, dtype=np.float64) * 2.0 / head_dim)
    freq = jnp.asarray(np.concatenate([half, half]).astype(np.float32)).reshape(1, head_dim)
    vmem = pl.BlockSpec(memory_space=pltpu.VMEM)
    hbm = pl.BlockSpec(memory_space=pl.ANY)
    dma = pltpu.SemaphoreType.DMA
    return pl.pallas_call(
        functools.partial(project_body, seq_count, q_heads, kv_heads, head_dim),
        out_shape=[
            jax.ShapeDtypeStruct((seq_count * q_heads, head_dim), F32),
            jax.ShapeDtypeStruct((seq_count * 2 * kv_heads, head_dim), F32),
        ],
        in_specs=[vmem, vmem, vmem, vmem, hbm, hbm, hbm],
        out_specs=[vmem, vmem],
        scratch_shapes=[
            pltpu.VMEM((seq_count, dim), BF16),
            pltpu.VMEM((chunks, dim, width), BF16),
            pltpu.VMEM((chunks, seq_count, width), F32),
            pltpu.VMEM((chunks, seq_count, width), F32),
            dma((chunks, splits)), dma((chunks,)), dma((chunks,)),
        ],
        compiler_params=pltpu.CompilerParams(collective_id=0, has_side_effects=True, vmem_limit_bytes=60 * 1024 * 1024),
        name="project",
    )(tokens, gains, positions.reshape(1, -1), freq, w_q, w_k, w_v)


def attn_body(seqs, slots, kv_heads, q_heads, pos_ref, start_ref, q_ref, kv_ref, k_ref, v_ref, ko_ref, vo_ref, o_ref, ml_ref, sc_ref, pw_ref):
    head_dim = q_ref.shape[-1]
    step = pl.program_id(0)
    scale = head_dim ** -0.5
    cols = slots * kv_heads
    group = q_heads // kv_heads
    row_id = lax.broadcasted_iota(jnp.int32, (q_heads, cols), 0)
    col_id = lax.broadcasted_iota(jnp.int32, (q_heads, cols), 1)
    own_head = jnp.zeros((q_heads, cols), jnp.int32)
    for h in range(1, kv_heads):
        own_head += (row_id >= h * group).astype(jnp.int32)
    slot_of = jnp.where(lax.rem(col_id, kv_heads) == own_head, lax.div(col_id, kv_heads), 1 << 20)
    upper = lax.broadcasted_iota(jnp.int32, (2 * kv_heads, head_dim), 0) >= kv_heads
    diag_r = lax.broadcasted_iota(jnp.int32, (q_heads, head_dim), 0)
    diag_c = lax.broadcasted_iota(jnp.int32, (q_heads, head_dim), 1)
    diag = diag_r == diag_c
    for b in range(seqs):
        rel = pos_ref[step * seqs + b] - start_ref[0]
        ko_ref[b] = k_ref[b]
        vo_ref[b] = v_ref[b]

        @pl.when((rel >= 0) & (rel < slots))
        def _():
            tile = lax.div(rel, 2)
            hit = upper == (lax.rem(rel, 2) == 1)
            k_new = kv_ref[pl.ds(b * 2 * kv_heads, kv_heads), :]
            v_new = kv_ref[pl.ds(b * 2 * kv_heads + kv_heads, kv_heads), :]
            k_two = jnp.concatenate([k_new, k_new], axis=0)
            v_two = jnp.concatenate([v_new, v_new], axis=0)
            ko_ref[b, tile] = jnp.where(hit, k_two, ko_ref[b, tile].astype(F32)).astype(BF16)
            vo_ref[b, tile] = jnp.where(hit, v_two, vo_ref[b, tile].astype(F32)).astype(BF16)

    peaks = []
    for b in range(seqs):
        rel = pos_ref[step * seqs + b] - start_ref[0]
        keys = ko_ref[b].reshape(cols, head_dim)
        query = q_ref[pl.ds(b * q_heads, q_heads), :].astype(BF16)
        scores = lax.dot_general(query, keys, (((1,), (1,)), ((), ())), preferred_element_type=F32) * scale
        scores = jnp.where(slot_of <= rel, scores, -jnp.inf)
        sc_ref[b] = scores
        peaks.append(jnp.max(scores, axis=1, keepdims=True))
    totals = []
    for b in range(seqs):
        rel = pos_ref[step * seqs + b] - start_ref[0]
        shift = jnp.where(rel < 0, 0.0, peaks[b])
        weights = jnp.exp(sc_ref[b] - shift)
        totals.append(jnp.sum(weights, axis=1, keepdims=True))
        pw_ref[b] = weights.astype(BF16)
    for b in range(seqs):
        vals = vo_ref[b].reshape(cols, head_dim)
        o_ref[pl.ds(b * q_heads, q_heads), :] = jnp.dot(pw_ref[b], vals, preferred_element_type=F32)
        peak = jnp.maximum(peaks[b], NEG_FILL)
        ml_ref[0, 0, pl.ds(b, 1), :] = jnp.sum(jnp.where(diag, peak, 0.0), axis=0, keepdims=True)
        ml_ref[0, 1, pl.ds(b, 1), :] = jnp.sum(jnp.where(diag, totals[b], 0.0), axis=0, keepdims=True)


def attention(q_rows, kv_rows, positions, shard_start, k_cache, v_cache):
    seq_count, slots, kv_heads, head_dim = k_cache.shape
    q_heads = q_rows.shape[0] // seq_count
    seqs = 8
    steps = seq_count // seqs
    pairs = slots // 2
    k4 = k_cache.reshape(seq_count, pairs, 2 * kv_heads, head_dim)
    v4 = v_cache.reshape(seq_count, pairs, 2 * kv_heads, head_dim)
    cache_block = pl.BlockSpec((seqs, pairs, 2 * kv_heads, head_dim), lambda i, *_: (i, 0, 0, 0))
    grid_spec = pltpu.PrefetchScalarGridSpec(
        num_scalar_prefetch=2,
        grid=(steps,),
        in_specs=[
            pl.BlockSpec((seqs * q_heads, head_dim), lambda i, *_: (i, 0)),
            pl.BlockSpec((seqs * 2 * kv_heads, head_dim), lambda i, *_: (i, 0)),
            cache_block,
            cache_block,
        ],
        out_specs=[
            cache_block,
            cache_block,
            pl.BlockSpec((seqs * q_heads, head_dim), lambda i, *_: (i, 0)),
            pl.BlockSpec((1, 2, seqs, head_dim), lambda i, *_: (i, 0, 0, 0)),
        ],
        scratch_shapes=[
            pltpu.VMEM((seqs, q_heads, slots * kv_heads), F32),
            pltpu.VMEM((seqs, q_heads, slots * kv_heads), BF16),
        ],
    )
    k_out, v_out, part, ml = pl.pallas_call(
        functools.partial(attn_body, seqs, slots, kv_heads, q_heads),
        grid_spec=grid_spec,
        out_shape=[
            jax.ShapeDtypeStruct(k4.shape, BF16),
            jax.ShapeDtypeStruct(v4.shape, BF16),
            jax.ShapeDtypeStruct((seq_count * q_heads, head_dim), F32),
            jax.ShapeDtypeStruct((steps, 2, seqs, head_dim), F32),
        ],
        compiler_params=pltpu.CompilerParams(dimension_semantics=("arbitrary",)),
        name="attend",
    )(positions, shard_start, q_rows, kv_rows, k4, v4)
    return k_out.reshape(k_cache.shape), v_out.reshape(v_cache.shape), part, ml


def blend(parts, stats, seqs, q_heads, row0=0):
    peak = stats[0][0]
    for m, _ in stats[1:]:
        peak = jnp.maximum(peak, m)
    factors = [jnp.exp(m - peak) for m, _ in stats]
    total = factors[0] * stats[0][1]
    for f, (_, l) in zip(factors[1:], stats[1:]):
        total += f * l
    return peak, total, factors


def columns_of(tile):
    return jnp.transpose(tile)


def combine_body(side, q_heads, o_ref, ml_ref, wo_ref, out_ref,
                 r1, rm1, s1, sm1, r2, rm2, s2, sm2, r3, rm3, obuf, lhs, wbuf, gbuf,
                 w_sem, a_s, a_r, b_s, b_r, c_s, c_r, d_s, d_r, e_s, e_r, f_s, f_r, h_s, h_r):
    me = lax.axis_index("sp")
    core = lax.rem(me, 2)
    chip = lax.div(me, 2)
    x = lax.rem(chip, side)
    y = lax.div(chip, side)
    first = x * (1 - core) + y * core
    second = y * (1 - core) + x * core
    stride1 = 2 * (1 - core) + 2 * side * core
    stride2 = 2 * side * (1 - core) + 2 * core
    partner = me + 1 - 2 * core
    head_dim = o_ref.shape[-1]
    width = wbuf.shape[1]
    depth = wbuf.shape[0]
    w_parts = w_sem.shape[0]
    w_rows = depth // w_parts
    order = [side // 2] + [d for d in range(1, side) if d != side // 2]

    def peer1(d):
        return me + (lax.rem(first + d, side) - first) * stride1

    def peer2(d):
        return me + (lax.rem(second + d, side) - second) * stride2

    def send(src, dst, ssem, rsem, to):
        copy = pltpu.make_async_remote_copy(src_ref=src, dst_ref=dst, send_sem=ssem, recv_sem=rsem, device_id={"sp": to}, device_id_type=MESH)
        copy.start()
        return copy

    w_copies = []
    for i in range(w_parts):
        copy = pltpu.make_async_copy(
            wo_ref.at[pl.ds(i * w_rows, w_rows), pl.ds(pl.multiple_of(core * width, 128), width)],
            wbuf.at[pl.ds(i * w_rows, w_rows), :], w_sem.at[i])
        copy.start()
        w_copies.append(copy)

    barrier = pltpu.get_barrier_semaphore()
    neighbours = [partner] + [peer1(d) for d in range(1, side)] + [peer2(d) for d in range(1, side)]
    for n in neighbours:
        pl.semaphore_signal(barrier, inc=1, device_id={"sp": n}, device_id_type=MESH)
    pl.semaphore_wait(barrier, len(neighbours))

    started = []
    in1 = {}
    for d in order + [0]:
        piece = lax.rem(second + d, side)
        in1[d] = (send(o_ref.at[1 - core, piece], r1.at[d], a_s.at[d, 0], a_r.at[d, 0], partner),
                  send(ml_ref.at[1 - core, piece], rm1.at[d], a_s.at[d, 1], a_r.at[d, 1], partner))
    in2 = {}
    for d in order + [0]:
        in1[d][0].wait_recv()
        in1[d][1].wait_recv()
        piece = lax.rem(first + d, side)
        own_m, own_l = ml_ref[core, piece, 0], ml_ref[core, piece, 1]
        peak, total, fac = blend(None, [(own_m, own_l), (rm1[d, 0], rm1[d, 1])], None, None)
        sm1[d, 0] = peak
        sm1[d, 1] = total
        cols = [columns_of(f) for f in fac]
        for k in range(side):
            for i in range(2):
                seq = 2 * k + i
                rows = pl.ds(i * q_heads, q_heads)
                s1[d, k, rows, :] = (o_ref[core, piece, k, rows, :] * cols[0][:q_heads, seq:seq + 1]
                                     + r1[d, k, rows, :] * cols[1][:q_heads, seq:seq + 1])
        if d:
            in2[d] = (send(s1.at[d], r2.at[d], b_s.at[d, 0], b_r.at[d, 0], peer1(d)),
                      send(sm1.at[d], rm2.at[d], b_s.at[d, 1], b_r.at[d, 1], peer1(d)))
    for d in order:
        in2[d][0].wait_recv()
        in2[d][1].wait_recv()
    stats = [(sm1[0, 0], sm1[0, 1])] + [(rm2[d, 0], rm2[d, 1]) for d in range(1, side)]
    peak, total, fac = blend(None, stats, None, None)
    sm2[0] = peak
    sm2[1] = total
    cols = [columns_of(f) for f in fac]
    for k in range(side):
        for i in range(2):
            seq = 2 * k + i
            rows = pl.ds(i * q_heads, q_heads)
            value = s1[0, k, rows, :] * cols[0][:q_heads, seq:seq + 1]
            for d in range(1, side):
                value += r2[d, k, rows, :] * cols[d][:q_heads, seq:seq + 1]
            s2[k, rows, :] = value
    in3 = {}
    for d in order:
        in3[d] = (send(s2.at[lax.rem(second + d, side)], r3.at[d], c_s.at[d, 0], c_r.at[d, 0], peer2(d)),
                  send(sm2, rm3.at[d], c_s.at[d, 1], c_r.at[d, 1], peer2(d)))
    for d in order:
        in3[d][0].wait_recv()
        in3[d][1].wait_recv()
    stats = [(sm2[0], sm2[1])] + [(rm3[d, 0], rm3[d, 1]) for d in range(1, side)]
    peak, total, fac = blend(None, stats, None, None)
    rm3[0, 0] = total
    for d in range(side):
        rm3[d, 1] = fac[d]
    mine = pl.ds(2 * second, 2)
    cols = []
    for d in range(side):
        cols.append(columns_of(jnp.concatenate([rm3[d, 1, mine, :]] * 4, axis=0)))
    l_cols = columns_of(jnp.concatenate([rm3[0, 0, mine, :]] * 4, axis=0))
    for i in range(2):
        rows = pl.ds(i * q_heads, q_heads)
        value = s2[second, rows, :] * cols[0][:q_heads, i:i + 1]
        for d in range(1, side):
            value += r3[d, rows, :] * cols[d][:q_heads, i:i + 1]
        value = value / l_cols[:q_heads, i:i + 1]
        obuf[core, rows, :] = value.astype(BF16).astype(F32)
    swap = send(obuf.at[core], obuf.at[core], d_s, d_r, partner)
    swap.wait_recv()

    for i in range(2):
        for h in range(q_heads):
            lhs[i:i + 1, h * head_dim:(h + 1) * head_dim] = obuf[0, i * q_heads + h:i * q_heads + h + 1, :]
            lhs[2 + i:3 + i, h * head_dim:(h + 1) * head_dim] = obuf[1, i * q_heads + h:i * q_heads + h + 1, :]
    for copy in w_copies:
        copy.wait()
    left = lhs[...].astype(BF16)

    def pair_a(f, s):
        return (f * side + s) * (1 - core) + (s * side + f) * core

    def pair_b(f, s):
        return side * side + (s * side + f) * (1 - core) + (f * side + s) * core

    pa, pb = pair_a(first, second), pair_b(first, second)
    n_step = 512
    for n in range(0, width, n_step):
        prod = jnp.dot(left, wbuf[:, n:n + n_step], preferred_element_type=F32)
        gbuf[core, pa, :, n:n + n_step] = prod[0:2]
        gbuf[core, pb, :, n:n + n_step] = prod[2:4]

    g1, g2, g3 = {}, {}, {}
    for d in order:
        for ab, p in enumerate((pa, pb)):
            g1[d, ab] = send(gbuf.at[core, p], gbuf.at[core, p], e_s.at[d, ab], e_r.at[d, ab], peer1(d))
    for ab, p in enumerate((pa, pb)):
        for e in order:
            g2[e, 0, ab] = send(gbuf.at[core, p], gbuf.at[core, p], f_s.at[e, 0, ab], f_r.at[e, 0, ab], peer2(e))
        g3[0, 0, ab] = send(gbuf.at[core, p], gbuf.at[core, p], h_s.at[0, 0, ab], h_r.at[0, 0, ab], partner)
    for d in order:
        f_from = lax.rem(first - d + side, side)
        for ab, p in enumerate((pair_a(f_from, second), pair_b(f_from, second))):
            g1[d, ab].wait_recv()
            for e in order:
                g2[e, d, ab] = send(gbuf.at[core, p], gbuf.at[core, p], f_s.at[e, d, ab], f_r.at[e, d, ab], peer2(e))
            g3[0, d, ab] = send(gbuf.at[core, p], gbuf.at[core, p], h_s.at[0, d, ab], h_r.at[0, d, ab], partner)
    for d in [0] + order:
        f_from = lax.rem(first - d + side, side)
        for e in order:
            s_from = lax.rem(second - e + side, side)
            for ab, p in enumerate((pair_a(f_from, s_from), pair_b(f_from, s_from))):
                g2[e, d, ab].wait_recv()
                g3[e, d, ab] = send(gbuf.at[core, p], gbuf.at[core, p], h_s.at[e, d, ab], h_r.at[e, d, ab], partner)
    for key in g3:
        g3[key].wait_recv()
    for half in range(2):
        for p in range(2 * side * side):
            out_ref[2 * p:2 * p + 2, half * width:(half + 1) * width] = gbuf[half, p]

    for group in (in1, in2, in3):
        for pair in group.values():
            pair[0].wait_send()
            pair[1].wait_send()
    swap.wait_send()
    for group in (g1, g2, g3):
        for copy in group.values():
            copy.wait_send()


def combine(part, ml, tokens, w_o, side):
    seq_count, dim = tokens.shape
    head_dim = part.shape[-1]
    q_heads = part.shape[0] // seq_count
    rows = 2 * q_heads
    o5 = part.reshape(2, side, side, rows, head_dim)
    m5 = ml.reshape(2, side, 2, ml.shape[2], head_dim)
    width = dim // 2
    depth = w_o.shape[0]
    dma = pltpu.SemaphoreType.DMA
    vmem = pl.BlockSpec(memory_space=pltpu.VMEM)
    piece = (side, side, rows, head_dim)
    stat = (side, 2, ml.shape[2], head_dim)
    return pl.pallas_call(
        functools.partial(combine_body, side, q_heads),
        out_shape=jax.ShapeDtypeStruct(tokens.shape, F32),
        in_specs=[vmem, vmem, pl.BlockSpec(memory_space=pl.ANY)],
        out_specs=vmem,
        scratch_shapes=[
            pltpu.VMEM(piece, F32), pltpu.VMEM(stat, F32),
            pltpu.VMEM(piece, F32), pltpu.VMEM(stat, F32),
            pltpu.VMEM(piece, F32), pltpu.VMEM(stat, F32),
            pltpu.VMEM(piece[1:], F32), pltpu.VMEM(stat[1:], F32),
            pltpu.VMEM(piece[1:], F32), pltpu.VMEM(stat, F32),
            pltpu.VMEM((2, rows, head_dim), F32),
            pltpu.VMEM((8, depth), F32),
            pltpu.VMEM((depth, width), BF16),
            pltpu.VMEM((2, 2 * side * side, 2, width), F32),
            dma((4,)),
            dma((side, 2)), dma((side, 2)),
            dma((side, 2)), dma((side, 2)),
            dma((side, 2)), dma((side, 2)),
            dma, dma,
            dma((side, 2)), dma((side, 2)),
            dma((side, side, 2)), dma((side, side, 2)),
            dma((side, side, 2)), dma((side, side, 2)),
        ],
        compiler_params=pltpu.CompilerParams(collective_id=1, has_side_effects=True, vmem_limit_bytes=60 * 1024 * 1024),
        name="combine",
    )(o5, m5, w_o)


def solution(mesh):
    cache_spec = P('dp', 'sp', None, None)
    side = int(round((mesh.shape['sp'] // 2) ** 0.5))

    def device_step(tokens, positions, k_cache, v_cache, w_q, w_k, w_v, w_o, attn_norm, q_norm, k_norm):
        seq_count, slots, kv_heads, head_dim = k_cache.shape
        shard_start = (lax.axis_index('sp') * slots).astype(jnp.int32).reshape(1)
        q_rows, kv_rows = project(tokens, positions, w_q, w_k, w_v, attn_norm, q_norm, k_norm)
        new_kv = kv_rows.astype(BF16).reshape(seq_count, 2, kv_heads, head_dim)
        k_upd, v_upd, part, ml = attention(q_rows, kv_rows, positions, shard_start, k_cache, v_cache)
        mixed = combine(part, ml, tokens, w_o, side)
        block_out = (tokens.astype(F32) + mixed).astype(BF16)
        return block_out, k_upd, v_upd, new_kv

    return jax.shard_map(device_step, mesh=mesh, in_specs=(P('dp', None), P('dp'), cache_spec, cache_spec, P(), P(), P(), P(), P(), P(), P()), out_specs=(P('dp', None), cache_spec, cache_spec, P('dp', None, None, None)), check_vma=False)
```

```python
import functools

import jax
import jax.numpy as jnp
import numpy as np
from jax import lax
from jax.experimental import pallas as pl
from jax.experimental.pallas import tpu as pltpu
from jax.sharding import PartitionSpec as P

NORM_EPS = 1e-6
ROPE_THETA = 1000000.0
NEG_FILL = -1e30
MESH = pl.DeviceIdType.MESH
F32 = jnp.float32
BF16 = jnp.bfloat16
MIB = 1024 * 1024
LIMIT_A = 27 * MIB
LIMIT_B = 28 * MIB
LIMIT_C = 37 * MIB


def project_body(seq_count, q_heads, kv_heads, head_dim, tok_ref, gain_ref, qn_ref, kn_ref, pos_ref, freq_ref, wq_ref, wk_ref, wv_ref,
                 heads, tok, hid, wbuf, w_sem, t_sem, s_sem, r_sem):
    me = lax.axis_index("sp")
    core = lax.rem(me, 2)
    partner = me + 1 - 2 * core
    dim = tok_ref.shape[1]
    slots, _, width = wbuf.shape
    chunks = w_sem.shape[0]
    per = width // head_dim
    splits = w_sem.shape[1]
    rows = dim // splits
    kv_chunks = kv_heads // 2 // per

    def first_head(i, side):
        if i < kv_chunks:
            return side * (kv_heads // 2) + i * per, wk_ref, side * (kv_heads // 2) + i * per
        if i < 2 * kv_chunks:
            own = side * (kv_heads // 2) + (i - kv_chunks) * per
            return kv_heads + own, wv_ref, own
        own = side * (q_heads // 2) + (i - 2 * kv_chunks) * per
        return 2 * kv_heads + own, wq_ref, own

    def fetch(i, j):
        _, ref, head = first_head(i, core)
        return pltpu.make_async_copy(
            ref.at[pl.ds(j * rows, rows), pl.ds(pl.multiple_of(head * head_dim, 128), width)],
            wbuf.at[i % slots, pl.ds(j * rows, rows), :], w_sem.at[i, j])

    load = pltpu.make_async_copy(tok_ref, tok, t_sem)
    load.start()
    pieces = [(i, j) for i in range(chunks) for j in range(splits)]
    ahead = 3
    for i, j in pieces[:ahead]:
        fetch(i, j).start()

    barrier = pltpu.get_barrier_semaphore()
    pl.semaphore_signal(barrier, inc=1, device_id={"sp": partner}, device_id_type=MESH)

    eye = lax.broadcasted_iota(jnp.int32, (seq_count, seq_count), 0) == lax.broadcasted_iota(jnp.int32, (seq_count, seq_count), 1)
    pos = jnp.sum(jnp.where(eye, pos_ref[...].astype(F32), 0.0), axis=1, keepdims=True)
    angles = pos * freq_ref[...]
    cos = jnp.cos(angles)
    lower = lax.broadcasted_iota(jnp.int32, (seq_count, head_dim), 1) < head_dim // 2
    sin = jnp.sin(angles)
    sin = jnp.where(lower, -sin, sin)
    q_gain = qn_ref[...].astype(F32)
    k_gain = kn_ref[...].astype(F32)
    load.wait()
    values = tok[...].astype(F32)
    scale = lax.rsqrt(jnp.mean(values * values, axis=-1, keepdims=True) + NORM_EPS)
    for j in range(dim // 128):
        at = slice(j * 128, (j + 1) * 128)
        hid[:, at] = (tok[:, at].astype(F32) * scale * gain_ref[j:j + 1, :].astype(F32)).astype(BF16)
    pl.semaphore_wait(barrier, 1)

    swaps = []
    blocks, _, block, _ = heads.shape
    for i in range(chunks):
        acc = None
        for j in range(splits):
            at = i * splits + j
            fetch(i, j).wait()
            if at + ahead < len(pieces):
                fetch(*pieces[at + ahead]).start()
            part = jnp.dot(hid[:, j * rows:(j + 1) * rows], wbuf[i % slots, j * rows:(j + 1) * rows, :], preferred_element_type=F32)
            acc = part if acc is None else acc + part
        acc = acc.astype(BF16).astype(F32)
        at = first_head(i, core)[0]
        for n in range(per):
            value = acc[:, n * head_dim:(n + 1) * head_dim]
            if not kv_chunks <= i < 2 * kv_chunks:
                scale = lax.rsqrt(jnp.mean(value * value, axis=-1, keepdims=True) + NORM_EPS)
                value = value * scale * (k_gain if i < kv_chunks else q_gain)
                value = value * cos + pltpu.roll(value, head_dim // 2, 1) * sin
                value = value.astype(BF16).astype(F32)
            for m in range(blocks):
                heads[m, at + n] = value[m * block:(m + 1) * block]
        span = heads.at[:, pl.ds(at, per)]
        copy = pltpu.make_async_remote_copy(
            src_ref=span, dst_ref=span, send_sem=s_sem.at[i], recv_sem=r_sem.at[i],
            device_id={"sp": partner}, device_id_type=MESH)
        copy.start()
        swaps.append(copy)
    for copy in swaps:
        copy.wait()


def project(seqs, tokens, positions, w_q, w_k, w_v, attn_norm, q_norm, k_norm):
    seq_count, dim = tokens.shape
    head_dim = q_norm.shape[0]
    q_heads = w_q.shape[1] // head_dim
    kv_heads = w_k.shape[1] // head_dim
    width = 4 * head_dim
    chunks = (w_q.shape[1] + w_k.shape[1] + w_v.shape[1]) // 2 // width
    splits = 2
    half = ROPE_THETA ** (-np.arange(head_dim // 2, dtype=np.float64) * 2.0 / head_dim)
    freq = jnp.asarray(np.concatenate([half, half]).astype(np.float32)).reshape(1, head_dim)
    vmem = pl.BlockSpec(memory_space=pltpu.VMEM)
    hbm = pl.BlockSpec(memory_space=pl.ANY)
    dma = pltpu.SemaphoreType.DMA
    return pl.pallas_call(
        functools.partial(project_body, seq_count, q_heads, kv_heads, head_dim),
        out_shape=jax.ShapeDtypeStruct((seq_count // seqs, q_heads + 2 * kv_heads, seqs, head_dim), F32),
        in_specs=[hbm, vmem, vmem, vmem, vmem, vmem, hbm, hbm, hbm],
        out_specs=vmem,
        scratch_shapes=[
            pltpu.VMEM((seq_count, dim), BF16),
            pltpu.VMEM((seq_count, dim), BF16),
            pltpu.VMEM((4, dim, width), BF16),
            dma((chunks, splits)), dma, dma((chunks,)), dma((chunks,)),
        ],
        compiler_params=pltpu.CompilerParams(collective_id=0, has_side_effects=True, vmem_limit_bytes=LIMIT_A),
        name="project",
    )(*[pltpu.with_memory_space_constraint(a, pltpu.HBM) for a in (
        tokens, attn_norm.reshape(-1, 128), q_norm.reshape(1, -1), k_norm.reshape(1, -1), positions.reshape(1, -1), freq, w_q, w_k, w_v)])


def attn_body(steps, seqs, slots, kv_heads, q_heads, pos_ref, start_ref, heads, k_ref, v_ref, ko_ref, vo_ref, obuf, nk_ref,
              kbuf, vbuf, nkbuf, sc_ref, pw_ref, o_sem):
    head_dim = k_ref.shape[-1]
    scale = head_dim ** -0.5
    cols = slots * kv_heads
    group = q_heads // kv_heads
    o_rows = seqs * q_heads

    def span(i):
        return pl.ds(i * seqs, seqs)

    def caches_out(i):
        slot = lax.rem(i, 2)
        return [
            pltpu.make_async_copy(kbuf.at[slot], ko_ref.at[span(i)], o_sem.at[i, 2]),
            pltpu.make_async_copy(vbuf.at[slot], vo_ref.at[span(i)], o_sem.at[i, 3]),
        ]

    def rest_out(i):
        return [
            pltpu.make_async_copy(nkbuf.at[span(i)], nk_ref.at[span(i)], o_sem.at[i, 1]),
        ]

    row_id = lax.broadcasted_iota(jnp.int32, (q_heads, cols), 0)
    col_id = lax.broadcasted_iota(jnp.int32, (q_heads, cols), 1)
    own_head = jnp.zeros((q_heads, cols), jnp.int32)
    for h in range(1, kv_heads):
        own_head += (row_id >= h * group).astype(jnp.int32)
    slot_of = jnp.where(lax.rem(col_id, kv_heads) == own_head, lax.div(col_id, kv_heads), 1 << 20)
    upper = lax.broadcasted_iota(jnp.int32, (2 * kv_heads, head_dim), 0) >= kv_heads
    diag_r = lax.broadcasted_iota(jnp.int32, (q_heads, head_dim), 0)
    diag_c = lax.broadcasted_iota(jnp.int32, (q_heads, head_dim), 1)
    diag = diag_r == diag_c

    @pl.loop(0, steps)
    def _(i):
        rows_of = heads.at[i].reshape((2 * kv_heads + q_heads) * seqs, head_dim)
        slot = lax.rem(i, 2)

        @pl.when(i >= 2)
        def _():
            for copy in caches_out(i - 2):
                copy.wait()

        for b in range(seqs):
            rel = pos_ref[i * seqs + b] - start_ref[0]
            at = i * seqs + b
            kbuf[slot, b] = k_ref[at]
            vbuf[slot, b] = v_ref[at]
            k_new = rows_of[pl.ds(b, kv_heads, stride=seqs), :]
            v_new = rows_of[pl.ds(b + kv_heads * seqs, kv_heads, stride=seqs), :]
            nkbuf[at] = jnp.concatenate([k_new, v_new], axis=0).astype(BF16)

            @pl.when((rel >= 0) & (rel < slots))
            def _():
                tile = lax.div(rel, 2)
                hit = upper == (lax.rem(rel, 2) == 1)
                k_two = jnp.concatenate([k_new, k_new], axis=0)
                v_two = jnp.concatenate([v_new, v_new], axis=0)
                kbuf[slot, b, tile] = jnp.where(hit, k_two, kbuf[slot, b, tile].astype(F32)).astype(BF16)
                vbuf[slot, b, tile] = jnp.where(hit, v_two, vbuf[slot, b, tile].astype(F32)).astype(BF16)
        for copy in caches_out(i):
            copy.start()
        peaks = []
        for b in range(seqs):
            rel = pos_ref[i * seqs + b] - start_ref[0]
            keys = kbuf[slot, b].reshape(cols, head_dim)
            query = rows_of[pl.ds(b + 2 * kv_heads * seqs, q_heads, stride=seqs), :].astype(BF16)
            scores = lax.dot_general(query, keys, (((1,), (1,)), ((), ())), preferred_element_type=F32) * scale
            scores = jnp.where(slot_of <= rel, scores, -jnp.inf)
            sc_ref[b] = scores
            peaks.append(jnp.max(scores, axis=1, keepdims=True))
        totals = []
        for b in range(seqs):
            rel = pos_ref[i * seqs + b] - start_ref[0]
            shift = jnp.where(rel < 0, 0.0, peaks[b])
            weights = jnp.exp(sc_ref[b] - shift)
            totals.append(jnp.sum(weights, axis=1, keepdims=True))
            pw_ref[b] = weights.astype(BF16)
        for b in range(seqs):
            vals = vbuf[slot, b].reshape(cols, head_dim)
            obuf[i, pl.ds(b * q_heads, q_heads), :] = jnp.dot(pw_ref[b], vals, preferred_element_type=F32)
            peak = jnp.maximum(peaks[b], NEG_FILL)
            obuf[i, pl.ds(o_rows + b, 1), :] = jnp.sum(jnp.where(diag, peak, 0.0), axis=0, keepdims=True)
            obuf[i, pl.ds(o_rows + seqs + b, 1), :] = jnp.sum(jnp.where(diag, totals[b], 0.0), axis=0, keepdims=True)
        for copy in rest_out(i):
            copy.start()

    for i in range(steps):
        for copy in rest_out(i) + (caches_out(i) if i >= steps - 2 else []):
            copy.wait()


def attention(seqs, heads, positions, shard_start, k_cache, v_cache):
    seq_count, slots, kv_heads, head_dim = k_cache.shape
    q_heads = heads.shape[1] - 2 * kv_heads
    steps = seq_count // seqs
    pairs = slots // 2
    part_rows = seqs * q_heads + 2 * seqs
    k4 = k_cache.reshape(seq_count, pairs, 2 * kv_heads, head_dim)
    v4 = v_cache.reshape(seq_count, pairs, 2 * kv_heads, head_dim)
    hbm = pl.BlockSpec(memory_space=pl.ANY)
    vmem = pl.BlockSpec(memory_space=pltpu.VMEM)
    smem = pl.BlockSpec(memory_space=pltpu.SMEM)
    dma = pltpu.SemaphoreType.DMA
    k_out, v_out, part, new_kv = pl.pallas_call(
        functools.partial(attn_body, steps, seqs, slots, kv_heads, q_heads),
        in_specs=[smem, smem, vmem, vmem, vmem],
        out_specs=[hbm, hbm, vmem, hbm],
        out_shape=[
            jax.ShapeDtypeStruct(k4.shape, BF16),
            jax.ShapeDtypeStruct(v4.shape, BF16),
            jax.ShapeDtypeStruct((steps, part_rows, head_dim), F32),
            jax.ShapeDtypeStruct((seq_count, 2 * kv_heads, head_dim), BF16),
        ],
        scratch_shapes=[
            pltpu.VMEM((2, seqs) + k4.shape[1:], BF16),
            pltpu.VMEM((2, seqs) + v4.shape[1:], BF16),
            pltpu.VMEM((seq_count, 2 * kv_heads, head_dim), BF16),
            pltpu.VMEM((seqs, q_heads, slots * kv_heads), F32),
            pltpu.VMEM((seqs, q_heads, slots * kv_heads), BF16),
            dma((steps, 4)),
        ],
        compiler_params=pltpu.CompilerParams(vmem_limit_bytes=LIMIT_B),
        name="attend",
    )(positions, shard_start, heads, k4, v4)
    return (k_out.reshape(k_cache.shape), v_out.reshape(v_cache.shape), part,
            new_kv.reshape(seq_count, 2, kv_heads, head_dim))


def blend(stats):
    peak = stats[0][0]
    for m, _ in stats[1:]:
        peak = jnp.maximum(peak, m)
    factors = [jnp.exp(m - peak) for m, _ in stats]
    total = factors[0] * stats[0][1]
    for f, (_, l) in zip(factors[1:], stats[1:]):
        total += f * l
    return peak, total, factors


def combine_body(side, q_heads, seqs, o_ref, wo_ref, out_ref, r1, s1, r2, s2, r3, fin, obuf, lhs, wbuf, gbuf,
                 w_sem, a_s, a_r, b_s, b_r, c_s, c_r, d_s, d_r, e_s, e_r, f_s, f_r, h_s, h_r):
    me = lax.axis_index("sp")
    core = lax.rem(me, 2)
    chip = lax.div(me, 2)
    x = lax.rem(chip, side)
    y = lax.div(chip, side)
    first = x * (1 - core) + y * core
    second = y * (1 - core) + x * core
    stride1 = 2 * (1 - core) + 2 * side * core
    stride2 = 2 * side * (1 - core) + 2 * core
    partner = me + 1 - 2 * core
    head_dim = o_ref.shape[-1]
    depth, width = wbuf.shape
    w_parts = w_sem.shape[0]
    w_rows = depth // w_parts
    rows = 2 * q_heads
    body = side * rows
    stat_m, stat_l = pl.ds(body, seqs), pl.ds(body + seqs, seqs)
    order = [side // 2] + [d for d in range(1, side) if d != side // 2]

    def peer1(d):
        return me + (lax.rem(first + d, side) - first) * stride1

    def peer2(d):
        return me + (lax.rem(second + d, side) - second) * stride2

    def send(src, dst, ssem, rsem, to):
        copy = pltpu.make_async_remote_copy(src_ref=src, dst_ref=dst, send_sem=ssem, recv_sem=rsem, device_id={"sp": to}, device_id_type=MESH)
        copy.start()
        return copy

    barrier = pltpu.get_barrier_semaphore()
    neighbours = [partner] + [peer1(d) for d in range(1, side)] + [peer2(d) for d in range(1, side)]
    for n in neighbours:
        pl.semaphore_signal(barrier, inc=1, device_id={"sp": n}, device_id_type=MESH)
    pl.semaphore_wait(barrier, len(neighbours))

    in1 = {}
    for d in order + [0]:
        in1[d] = send(o_ref.at[1 - core, lax.rem(second + d, side)], r1.at[d], a_s.at[d], a_r.at[d], partner)
    w_copies = []
    for i in range(w_parts):
        copy = pltpu.make_async_copy(
            wo_ref.at[pl.ds(i * w_rows, w_rows), pl.ds(pl.multiple_of(core * width, 128), width)],
            wbuf.at[pl.ds(i * w_rows, w_rows), :], w_sem.at[i])
        copy.start()
        w_copies.append(copy)
    in2 = {}
    for d in order + [0]:
        in1[d].wait_recv()
        piece = lax.rem(first + d, side)
        peak, total, fac = blend([(o_ref[core, piece, stat_m, :], o_ref[core, piece, stat_l, :]), (r1[d, stat_m, :], r1[d, stat_l, :])])
        s1[d, stat_m, :] = peak
        s1[d, stat_l, :] = total
        cols = [jnp.transpose(f) for f in fac]
        for seq in range(seqs):
            at = pl.ds(seq * q_heads, q_heads)
            s1[d, at, :] = (o_ref[core, piece, at, :] * cols[0][:q_heads, seq:seq + 1]
                            + r1[d, at, :] * cols[1][:q_heads, seq:seq + 1])
        if d:
            in2[d] = send(s1.at[d], r2.at[d], b_s.at[d], b_r.at[d], peer1(d))
    for d in order:
        in2[d].wait_recv()
    peak, total, fac = blend([(s1[0, stat_m, :], s1[0, stat_l, :])] + [(r2[d, stat_m, :], r2[d, stat_l, :]) for d in range(1, side)])
    cols = [jnp.transpose(f) for f in fac]
    for k in range(side):
        for i in range(2):
            seq = 2 * k + i
            at = pl.ds(seq * q_heads, q_heads)
            value = s1[0, at, :] * cols[0][:q_heads, seq:seq + 1]
            for d in range(1, side):
                value += r2[d, at, :] * cols[d][:q_heads, seq:seq + 1]
            s2[k, pl.ds(i * q_heads, q_heads), :] = value
        s2[k, pl.ds(rows, seqs), :] = peak
        s2[k, pl.ds(rows + seqs, seqs), :] = total
    in3 = {}
    for d in order:
        in3[d] = send(s2.at[lax.rem(second + d, side)], r3.at[d], c_s.at[d], c_r.at[d], peer2(d))
    for d in order:
        in3[d].wait_recv()
    low, high = pl.ds(rows, seqs), pl.ds(rows + seqs, seqs)
    peak, total, fac = blend([(s2[0, low, :], s2[0, high, :])] + [(r3[d, low, :], r3[d, high, :]) for d in range(1, side)])
    for n, tile in enumerate(fac + [total]):
        fin[n] = tile
    mine = pl.ds(2 * second, 2)
    cols = [jnp.transpose(jnp.concatenate([fin[n, mine, :]] * (seqs // 2), axis=0)) for n in range(side + 1)]
    for i in range(2):
        at = pl.ds(i * q_heads, q_heads)
        value = s2[second, at, :] * cols[0][:q_heads, i:i + 1]
        for d in range(1, side):
            value += r3[d, at, :] * cols[d][:q_heads, i:i + 1]
        value = value / cols[side][:q_heads, i:i + 1]
        obuf[pl.ds(pl.multiple_of(core * rows, 8) + i * q_heads, q_heads), :] = value.astype(BF16).astype(F32)
    own = obuf.at[pl.ds(pl.multiple_of(core * rows, 8), rows)]
    swap = send(own, own, d_s, d_r, partner)
    lhs[...] = jnp.zeros_like(lhs)
    for copy in w_copies:
        copy.wait()
    swap.wait_recv()
    for h in range(q_heads):
        lhs[0:4, h * head_dim:(h + 1) * head_dim] = obuf[pl.ds(h, 4, stride=q_heads), :]
    left = lhs[...].astype(BF16)
    n_step = 512
    for n in range(0, width, n_step):
        gbuf[core, second, first, :, n:n + n_step] = jnp.dot(left, wbuf[:, n:n + n_step], preferred_element_type=F32)[0:4]

    def block(s, f):
        return gbuf.at[core, s, f]

    g1, g2, g3 = {}, {}, {}
    for d in order:
        g1[d] = send(block(second, first), block(second, first), e_s.at[d], e_r.at[d], peer1(d))
    for e in order:
        g2[e, 0] = send(block(second, first), block(second, first), f_s.at[e, 0], f_r.at[e, 0], peer2(e))
    for d in order[1:] + order[:1]:
        f_from = lax.rem(first - d + side, side)
        g1[d].wait_recv()
        for e in order:
            g2[e, d] = send(block(second, f_from), block(second, f_from), f_s.at[e, d], f_r.at[e, d], peer2(e))
    g3[0] = send(gbuf.at[core, second], gbuf.at[core, second], h_s.at[0], h_r.at[0], partner)
    for e in order[1:] + order[:1]:
        s_from = lax.rem(second - e + side, side)
        for d in range(side):
            g2[e, d].wait_recv()
        g3[e] = send(gbuf.at[core, s_from], gbuf.at[core, s_from], h_s.at[e], h_r.at[e], partner)
    for key in g3:
        g3[key].wait_recv()
    for half in range(2):
        at = slice(half * width, (half + 1) * width)
        for s in range(side):
            for f in range(side):
                px, py = (f, s) if half == 0 else (s, f)
                a = 2 * (px * side + py)
                b = 2 * (side * side + py * side + px)
                out_ref[a:a + 2, at] = gbuf[half, s, f, 0:2]
                out_ref[b:b + 2, at] = gbuf[half, s, f, 2:4]

    for group in (in1, in2, in3, g1, g2, g3):
        for copy in group.values():
            copy.wait_send()
    swap.wait_send()


def combine(part, tokens, w_o, side):
    seq_count, dim = tokens.shape
    steps, part_rows, head_dim = part.shape
    seqs = seq_count // steps
    q_heads = part_rows // seqs - 2
    parts = part.reshape(2, side, part_rows, head_dim)
    width = dim // 2
    depth = w_o.shape[0]
    dma = pltpu.SemaphoreType.DMA
    hbm = pl.BlockSpec(memory_space=pl.ANY)
    piece = (side, part_rows, head_dim)
    small = (side, 2 * q_heads + 2 * seqs, head_dim)
    return pl.pallas_call(
        functools.partial(combine_body, side, q_heads, seqs),
        out_shape=jax.ShapeDtypeStruct(tokens.shape, F32),
        in_specs=[pl.BlockSpec(memory_space=pltpu.VMEM), hbm],
        out_specs=pl.BlockSpec(memory_space=pltpu.VMEM),
        scratch_shapes=[
            pltpu.VMEM(piece, F32), pltpu.VMEM(piece, F32), pltpu.VMEM(piece, F32),
            pltpu.VMEM(small, F32), pltpu.VMEM(small, F32),
            pltpu.VMEM((side + 1, seqs, head_dim), F32),
            pltpu.VMEM((4 * q_heads, head_dim), F32),
            pltpu.VMEM((8, depth), F32),
            pltpu.VMEM((depth, width), BF16),
            pltpu.VMEM((2, side, side, 4, width), F32),
            dma((4,)),
            dma((side,)), dma((side,)),
            dma((side,)), dma((side,)),
            dma((side,)), dma((side,)),
            dma, dma,
            dma((side,)), dma((side,)),
            dma((side, side)), dma((side, side)),
            dma((side,)), dma((side,)),
        ],
        compiler_params=pltpu.CompilerParams(collective_id=1, has_side_effects=True, vmem_limit_bytes=LIMIT_C),
        name="combine",
    )(parts, w_o)


def solution(mesh):
    cache_spec = P('dp', 'sp', None, None)
    side = int(round((mesh.shape['sp'] // 2) ** 0.5))

    def device_step(tokens, positions, k_cache, v_cache, w_q, w_k, w_v, w_o, attn_norm, q_norm, k_norm):
        seq_count, slots, kv_heads, head_dim = k_cache.shape
        shard_start = (lax.axis_index('sp') * slots).astype(jnp.int32).reshape(1)
        seqs = 8
        heads = project(seqs, tokens, positions, w_q, w_k, w_v, attn_norm, q_norm, k_norm)
        k_upd, v_upd, part, new_kv = attention(seqs, heads, positions, shard_start, k_cache, v_cache)
        mixed = combine(part, tokens, w_o, side)
        block_out = (tokens.astype(F32) + mixed).astype(BF16)
        return block_out, k_upd, v_upd, new_kv

    return jax.shard_map(device_step, mesh=mesh, in_specs=(P('dp', None), P('dp'), cache_spec, cache_spec, P(), P(), P(), P(), P(), P(), P()), out_specs=(P('dp', None), cache_spec, cache_spec, P('dp', None, None, None)), check_vma=False)
```

```python
import functools

import jax
import jax.numpy as jnp
import numpy as np
from jax import lax
from jax.experimental import pallas as pl
from jax.experimental.pallas import tpu as pltpu
from jax.sharding import PartitionSpec as P

NORM_EPS = 1e-6
ROPE_THETA = 1000000.0
NEG_FILL = -1e30
MESH = pl.DeviceIdType.MESH
F32 = jnp.float32
BF16 = jnp.bfloat16
MIB = 1024 * 1024
LIMIT_A = 27 * MIB
LIMIT_B = 28 * MIB
LIMIT_C = 37 * MIB


def project_body(seq_count, q_heads, kv_heads, head_dim, tok_ref, gain_ref, qn_ref, kn_ref, pos_ref, freq_ref, wq_ref, wk_ref, wv_ref,
                 heads, tok, hid, wbuf, w_sem, t_sem, s_sem, r_sem):
    me = lax.axis_index("sp")
    core = lax.rem(me, 2)
    partner = me + 1 - 2 * core
    dim = tok_ref.shape[1]
    slots, _, width = wbuf.shape
    chunks = w_sem.shape[0]
    per = width // head_dim
    splits = w_sem.shape[1]
    rows = dim // splits
    kv_chunks = kv_heads // 2 // per

    def first_head(i, side):
        if i < kv_chunks:
            return side * (kv_heads // 2) + i * per, wk_ref, side * (kv_heads // 2) + i * per
        if i < 2 * kv_chunks:
            own = side * (kv_heads // 2) + (i - kv_chunks) * per
            return kv_heads + own, wv_ref, own
        own = side * (q_heads // 2) + (i - 2 * kv_chunks) * per
        return 2 * kv_heads + own, wq_ref, own

    def fetch(i, j):
        _, ref, head = first_head(i, core)
        return pltpu.make_async_copy(
            ref.at[pl.ds(j * rows, rows), pl.ds(pl.multiple_of(head * head_dim, 128), width)],
            wbuf.at[i % slots, pl.ds(j * rows, rows), :], w_sem.at[i, j])

    load = pltpu.make_async_copy(tok_ref, tok, t_sem)
    load.start()
    pieces = [(i, j) for i in range(chunks) for j in range(splits)]
    ahead = 5
    for i, j in pieces[:ahead]:
        fetch(i, j).start()

    barrier = pltpu.get_barrier_semaphore()
    pl.semaphore_signal(barrier, inc=1, device_id={"sp": partner}, device_id_type=MESH)

    eye = lax.broadcasted_iota(jnp.int32, (seq_count, seq_count), 0) == lax.broadcasted_iota(jnp.int32, (seq_count, seq_count), 1)
    pos = jnp.sum(jnp.where(eye, pos_ref[...].astype(F32), 0.0), axis=1, keepdims=True)
    angles = pos * freq_ref[...]
    cos = jnp.cos(angles)
    lower = lax.broadcasted_iota(jnp.int32, (seq_count, head_dim), 1) < head_dim // 2
    sin = jnp.sin(angles)
    sin = jnp.where(lower, -sin, sin)
    q_gain = qn_ref[...].astype(F32)
    k_gain = kn_ref[...].astype(F32)
    load.wait()
    values = tok[...].astype(F32)
    scale = lax.rsqrt(jnp.mean(values * values, axis=-1, keepdims=True) + NORM_EPS)
    for j in range(dim // 128):
        at = slice(j * 128, (j + 1) * 128)
        hid[:, at] = (tok[:, at].astype(F32) * scale * gain_ref[j:j + 1, :].astype(F32)).astype(BF16)
    pl.semaphore_wait(barrier, 1)

    swaps = []
    blocks, _, block, _ = heads.shape
    for i in range(chunks):
        acc = None
        for j in range(splits):
            at = i * splits + j
            fetch(i, j).wait()
            if at + ahead < len(pieces):
                fetch(*pieces[at + ahead]).start()
            part = jnp.dot(hid[:, j * rows:(j + 1) * rows], wbuf[i % slots, j * rows:(j + 1) * rows, :], preferred_element_type=F32)
            acc = part if acc is None else acc + part
        acc = acc.astype(BF16).astype(F32)
        at = first_head(i, core)[0]
        for n in range(per):
            value = acc[:, n * head_dim:(n + 1) * head_dim]
            if not kv_chunks <= i < 2 * kv_chunks:
                scale = lax.rsqrt(jnp.mean(value * value, axis=-1, keepdims=True) + NORM_EPS)
                value = value * scale * (k_gain if i < kv_chunks else q_gain)
                value = value * cos + pltpu.roll(value, head_dim // 2, 1) * sin
                value = value.astype(BF16).astype(F32)
            for m in range(blocks):
                heads[m, at + n] = value[m * block:(m + 1) * block]
        span = heads.at[:, pl.ds(at, per)]
        copy = pltpu.make_async_remote_copy(
            src_ref=span, dst_ref=span, send_sem=s_sem.at[i], recv_sem=r_sem.at[i],
            device_id={"sp": partner}, device_id_type=MESH)
        copy.start()
        swaps.append(copy)
    for copy in swaps:
        copy.wait()


def project(seqs, tokens, positions, w_q, w_k, w_v, attn_norm, q_norm, k_norm):
    seq_count, dim = tokens.shape
    head_dim = q_norm.shape[0]
    q_heads = w_q.shape[1] // head_dim
    kv_heads = w_k.shape[1] // head_dim
    width = 4 * head_dim
    chunks = (w_q.shape[1] + w_k.shape[1] + w_v.shape[1]) // 2 // width
    splits = 2
    half = ROPE_THETA ** (-np.arange(head_dim // 2, dtype=np.float64) * 2.0 / head_dim)
    freq = jnp.asarray(np.concatenate([half, half]).astype(np.float32)).reshape(1, head_dim)
    vmem = pl.BlockSpec(memory_space=pltpu.VMEM)
    hbm = pl.BlockSpec(memory_space=pl.ANY)
    dma = pltpu.SemaphoreType.DMA
    return pl.pallas_call(
        functools.partial(project_body, seq_count, q_heads, kv_heads, head_dim),
        out_shape=jax.ShapeDtypeStruct((seq_count // seqs, q_heads + 2 * kv_heads, seqs, head_dim), F32),
        in_specs=[hbm, vmem, vmem, vmem, vmem, vmem, hbm, hbm, hbm],
        out_specs=vmem,
        scratch_shapes=[
            pltpu.VMEM((seq_count, dim), BF16),
            pltpu.VMEM((seq_count, dim), BF16),
            pltpu.VMEM((4, dim, width), BF16),
            dma((chunks, splits)), dma, dma((chunks,)), dma((chunks,)),
        ],
        compiler_params=pltpu.CompilerParams(collective_id=0, has_side_effects=True, vmem_limit_bytes=LIMIT_A),
        name="project",
    )(*[pltpu.with_memory_space_constraint(a, pltpu.HBM) for a in (
        tokens, attn_norm.reshape(-1, 128), q_norm.reshape(1, -1), k_norm.reshape(1, -1), positions.reshape(1, -1), freq, w_q, w_k, w_v)])


def attn_body(steps, seqs, slots, kv_heads, q_heads, pos_ref, start_ref, heads, k_ref, v_ref, ko_ref, vo_ref, obuf, nk_ref,
              kbuf, vbuf, nkbuf, sc_ref, pw_ref, o_sem):
    head_dim = k_ref.shape[-1]
    scale = head_dim ** -0.5
    cols = slots * kv_heads
    group = q_heads // kv_heads
    o_rows = seqs * q_heads

    def span(i):
        return pl.ds(i * seqs, seqs)

    def caches_out(i):
        slot = lax.rem(i, 2)
        return [
            pltpu.make_async_copy(kbuf.at[slot], ko_ref.at[span(i)], o_sem.at[i, 2]),
            pltpu.make_async_copy(vbuf.at[slot], vo_ref.at[span(i)], o_sem.at[i, 3]),
        ]

    def rest_out(i):
        return [
            pltpu.make_async_copy(nkbuf.at[span(i)], nk_ref.at[span(i)], o_sem.at[i, 1]),
        ]

    row_id = lax.broadcasted_iota(jnp.int32, (q_heads, cols), 0)
    col_id = lax.broadcasted_iota(jnp.int32, (q_heads, cols), 1)
    own_head = jnp.zeros((q_heads, cols), jnp.int32)
    for h in range(1, kv_heads):
        own_head += (row_id >= h * group).astype(jnp.int32)
    slot_of = jnp.where(lax.rem(col_id, kv_heads) == own_head, lax.div(col_id, kv_heads), 1 << 20)
    upper = lax.broadcasted_iota(jnp.int32, (2 * kv_heads, head_dim), 0) >= kv_heads
    diag_r = lax.broadcasted_iota(jnp.int32, (q_heads, head_dim), 0)
    diag_c = lax.broadcasted_iota(jnp.int32, (q_heads, head_dim), 1)
    diag = diag_r == diag_c

    @pl.loop(0, steps)
    def _(i):
        rows_of = heads.at[i].reshape((2 * kv_heads + q_heads) * seqs, head_dim)
        slot = lax.rem(i, 2)

        @pl.when(i >= 2)
        def _():
            for copy in caches_out(i - 2):
                copy.wait()

        for b in range(seqs):
            rel = pos_ref[i * seqs + b] - start_ref[0]
            at = i * seqs + b
            kbuf[slot, b] = k_ref[at]
            vbuf[slot, b] = v_ref[at]
            k_new = rows_of[pl.ds(b, kv_heads, stride=seqs), :]
            v_new = rows_of[pl.ds(b + kv_heads * seqs, kv_heads, stride=seqs), :]
            nkbuf[at] = jnp.concatenate([k_new, v_new], axis=0).astype(BF16)

            @pl.when((rel >= 0) & (rel < slots))
            def _():
                tile = lax.div(rel, 2)
                hit = upper == (lax.rem(rel, 2) == 1)
                k_two = jnp.concatenate([k_new, k_new], axis=0)
                v_two = jnp.concatenate([v_new, v_new], axis=0)
                kbuf[slot, b, tile] = jnp.where(hit, k_two, kbuf[slot, b, tile].astype(F32)).astype(BF16)
                vbuf[slot, b, tile] = jnp.where(hit, v_two, vbuf[slot, b, tile].astype(F32)).astype(BF16)
        for copy in caches_out(i):
            copy.start()
        peaks = []
        for b in range(seqs):
            rel = pos_ref[i * seqs + b] - start_ref[0]
            keys = kbuf[slot, b].reshape(cols, head_dim)
            query = rows_of[pl.ds(b + 2 * kv_heads * seqs, q_heads, stride=seqs), :].astype(BF16)
            scores = lax.dot_general(query, keys, (((1,), (1,)), ((), ())), preferred_element_type=F32) * scale
            scores = jnp.where(slot_of <= rel, scores, -jnp.inf)
            sc_ref[b] = scores
            peaks.append(jnp.max(scores, axis=1, keepdims=True))
        totals = []
        for b in range(seqs):
            rel = pos_ref[i * seqs + b] - start_ref[0]
            shift = jnp.where(rel < 0, 0.0, peaks[b])
            weights = jnp.exp(sc_ref[b] - shift)
            totals.append(jnp.sum(weights, axis=1, keepdims=True))
            pw_ref[b] = weights.astype(BF16)
        for b in range(seqs):
            vals = vbuf[slot, b].reshape(cols, head_dim)
            obuf[i, pl.ds(b * q_heads, q_heads), :] = jnp.dot(pw_ref[b], vals, preferred_element_type=F32)
            peak = jnp.maximum(peaks[b], NEG_FILL)
            obuf[i, pl.ds(o_rows + b, 1), :] = jnp.sum(jnp.where(diag, peak, 0.0), axis=0, keepdims=True)
            obuf[i, pl.ds(o_rows + seqs + b, 1), :] = jnp.sum(jnp.where(diag, totals[b], 0.0), axis=0, keepdims=True)
        for copy in rest_out(i):
            copy.start()

    for i in range(steps):
        for copy in rest_out(i) + (caches_out(i) if i >= steps - 2 else []):
            copy.wait()


def attention(seqs, heads, positions, shard_start, k_cache, v_cache):
    seq_count, slots, kv_heads, head_dim = k_cache.shape
    q_heads = heads.shape[1] - 2 * kv_heads
    steps = seq_count // seqs
    pairs = slots // 2
    part_rows = seqs * q_heads + 2 * seqs
    k4 = k_cache.reshape(seq_count, pairs, 2 * kv_heads, head_dim)
    v4 = v_cache.reshape(seq_count, pairs, 2 * kv_heads, head_dim)
    hbm = pl.BlockSpec(memory_space=pl.ANY)
    vmem = pl.BlockSpec(memory_space=pltpu.VMEM)
    smem = pl.BlockSpec(memory_space=pltpu.SMEM)
    dma = pltpu.SemaphoreType.DMA
    k_out, v_out, part, new_kv = pl.pallas_call(
        functools.partial(attn_body, steps, seqs, slots, kv_heads, q_heads),
        in_specs=[smem, smem, vmem, vmem, vmem],
        out_specs=[hbm, hbm, vmem, hbm],
        out_shape=[
            jax.ShapeDtypeStruct(k4.shape, BF16),
            jax.ShapeDtypeStruct(v4.shape, BF16),
            jax.ShapeDtypeStruct((steps, part_rows, head_dim), F32),
            jax.ShapeDtypeStruct((seq_count, 2 * kv_heads, head_dim), BF16),
        ],
        scratch_shapes=[
            pltpu.VMEM((2, seqs) + k4.shape[1:], BF16),
            pltpu.VMEM((2, seqs) + v4.shape[1:], BF16),
            pltpu.VMEM((seq_count, 2 * kv_heads, head_dim), BF16),
            pltpu.VMEM((seqs, q_heads, slots * kv_heads), F32),
            pltpu.VMEM((seqs, q_heads, slots * kv_heads), BF16),
            dma((steps, 4)),
        ],
        compiler_params=pltpu.CompilerParams(vmem_limit_bytes=LIMIT_B),
        name="attend",
    )(positions, shard_start, heads, k4, v4)
    return (k_out.reshape(k_cache.shape), v_out.reshape(v_cache.shape), part,
            new_kv.reshape(seq_count, 2, kv_heads, head_dim))


def blend(stats):
    peak = stats[0][0]
    for m, _ in stats[1:]:
        peak = jnp.maximum(peak, m)
    factors = [jnp.exp(m - peak) for m, _ in stats]
    total = factors[0] * stats[0][1]
    for f, (_, l) in zip(factors[1:], stats[1:]):
        total += f * l
    return peak, total, factors


def combine_body(side, q_heads, seqs, o_ref, wo_ref, out_ref, r1, s1, r2, s2, r3, fin, obuf, lhs, wbuf, gbuf0, gbuf1,
                 w_sem, a_s, a_r, b_s, b_r, c_s, c_r, d_s, d_r, e_s, e_r, f_s, f_r, h_s, h_r):
    me = lax.axis_index("sp")
    core = lax.rem(me, 2)
    chip = lax.div(me, 2)
    x = lax.rem(chip, side)
    y = lax.div(chip, side)
    first = x * (1 - core) + y * core
    second = y * (1 - core) + x * core
    stride1 = 2 * (1 - core) + 2 * side * core
    stride2 = 2 * side * (1 - core) + 2 * core
    partner = me + 1 - 2 * core
    head_dim = o_ref.shape[-1]
    gbufs = (gbuf0, gbuf1)
    depth, width = wbuf.shape
    w_parts = w_sem.shape[0]
    w_rows = depth // w_parts
    rows = 2 * q_heads
    body = side * rows
    stat_m, stat_l = pl.ds(body, seqs), pl.ds(body + seqs, seqs)
    order = [side // 2] + [d for d in range(1, side) if d != side // 2]

    def peer1(d):
        return me + (lax.rem(first + d, side) - first) * stride1

    def peer2(d):
        return me + (lax.rem(second + d, side) - second) * stride2

    def send(src, dst, ssem, rsem, to):
        copy = pltpu.make_async_remote_copy(src_ref=src, dst_ref=dst, send_sem=ssem, recv_sem=rsem, device_id={"sp": to}, device_id_type=MESH)
        copy.start()
        return copy

    barrier = pltpu.get_barrier_semaphore()
    neighbours = [partner] + [peer1(d) for d in range(1, side)] + [peer2(d) for d in range(1, side)]
    for n in neighbours:
        pl.semaphore_signal(barrier, inc=1, device_id={"sp": n}, device_id_type=MESH)
    pl.semaphore_wait(barrier, len(neighbours))

    in1 = {}
    for d in order + [0]:
        in1[d] = send(o_ref.at[1 - core, lax.rem(second + d, side)], r1.at[d], a_s.at[d], a_r.at[d], partner)
    w_copies = []
    for i in range(w_parts):
        copy = pltpu.make_async_copy(
            wo_ref.at[pl.ds(i * w_rows, w_rows), pl.ds(pl.multiple_of(core * width, 128), width)],
            wbuf.at[pl.ds(i * w_rows, w_rows), :], w_sem.at[i])
        copy.start()
        w_copies.append(copy)
    in2 = {}
    for d in order + [0]:
        in1[d].wait_recv()
        piece = lax.rem(first + d, side)
        peak, total, fac = blend([(o_ref[core, piece, stat_m, :], o_ref[core, piece, stat_l, :]), (r1[d, stat_m, :], r1[d, stat_l, :])])
        s1[d, stat_m, :] = peak
        s1[d, stat_l, :] = total
        cols = [jnp.transpose(f) for f in fac]
        for seq in range(seqs):
            at = pl.ds(seq * q_heads, q_heads)
            s1[d, at, :] = (o_ref[core, piece, at, :] * cols[0][:q_heads, seq:seq + 1]
                            + r1[d, at, :] * cols[1][:q_heads, seq:seq + 1])
        if d:
            in2[d] = send(s1.at[d], r2.at[d], b_s.at[d], b_r.at[d], peer1(d))
    for d in order:
        in2[d].wait_recv()
    peak, total, fac = blend([(s1[0, stat_m, :], s1[0, stat_l, :])] + [(r2[d, stat_m, :], r2[d, stat_l, :]) for d in range(1, side)])
    cols = [jnp.transpose(f) for f in fac]
    for k in range(side):
        for i in range(2):
            seq = 2 * k + i
            at = pl.ds(seq * q_heads, q_heads)
            value = s1[0, at, :] * cols[0][:q_heads, seq:seq + 1]
            for d in range(1, side):
                value += r2[d, at, :] * cols[d][:q_heads, seq:seq + 1]
            s2[k, pl.ds(i * q_heads, q_heads), :] = value
        s2[k, pl.ds(rows, seqs), :] = peak
        s2[k, pl.ds(rows + seqs, seqs), :] = total
    in3 = {}
    for d in order:
        in3[d] = send(s2.at[lax.rem(second + d, side)], r3.at[d], c_s.at[d], c_r.at[d], peer2(d))
    for d in order:
        in3[d].wait_recv()
    low, high = pl.ds(rows, seqs), pl.ds(rows + seqs, seqs)
    peak, total, fac = blend([(s2[0, low, :], s2[0, high, :])] + [(r3[d, low, :], r3[d, high, :]) for d in range(1, side)])
    for n, tile in enumerate(fac + [total]):
        fin[n] = tile
    mine = pl.ds(2 * second, 2)
    cols = [jnp.transpose(jnp.concatenate([fin[n, mine, :]] * (seqs // 2), axis=0)) for n in range(side + 1)]
    for i in range(2):
        at = pl.ds(i * q_heads, q_heads)
        value = s2[second, at, :] * cols[0][:q_heads, i:i + 1]
        for d in range(1, side):
            value += r3[d, at, :] * cols[d][:q_heads, i:i + 1]
        value = value / cols[side][:q_heads, i:i + 1]
        obuf[pl.ds(pl.multiple_of(core * rows, 8) + i * q_heads, q_heads), :] = value.astype(BF16).astype(F32)
    own = obuf.at[pl.ds(pl.multiple_of(core * rows, 8), rows)]
    swap = send(own, own, d_s, d_r, partner)
    lhs[...] = jnp.zeros_like(lhs)
    for copy in w_copies:
        copy.wait()
    swap.wait_recv()
    for h in range(q_heads):
        lhs[0:4, h * head_dim:(h + 1) * head_dim] = obuf[pl.ds(h, 4, stride=q_heads), :]
    left = lhs[...].astype(BF16)
    g1, g2, g3 = {}, {}, {}
    n_step = 512
    done = 0
    for q, gbuf in enumerate(gbufs):
        own = gbuf.at[core, second, first]
        for n in range(0, gbuf.shape[-1], n_step):
            gbuf[core, second, first, :, n:n + n_step] = jnp.dot(left, wbuf[:, done + n:done + n + n_step], preferred_element_type=F32)[0:4]
        done += gbuf.shape[-1]
        for d in order:
            g1[q, d] = send(own, own, e_s.at[q, d], e_r.at[q, d], peer1(d))
        for e in order:
            g2[q, e, 0] = send(own, own, f_s.at[q, e, 0], f_r.at[q, e, 0], peer2(e))
    for q, gbuf in enumerate(gbufs):
        for d in order[1:] + order[:1]:
            f_from = lax.rem(first - d + side, side)
            got = gbuf.at[core, second, f_from]
            g1[q, d].wait_recv()
            for e in order:
                g2[q, e, d] = send(got, got, f_s.at[q, e, d], f_r.at[q, e, d], peer2(e))
        row = gbuf.at[core, second]
        g3[q, 0] = send(row, row, h_s.at[q, 0], h_r.at[q, 0], partner)
    for q, gbuf in enumerate(gbufs):
        for e in order[1:] + order[:1]:
            row = gbuf.at[core, lax.rem(second - e + side, side)]
            for d in range(side):
                g2[q, e, d].wait_recv()
            g3[q, e] = send(row, row, h_s.at[q, e], h_r.at[q, e], partner)
    done = 0
    for q, gbuf in enumerate(gbufs):
        for e in range(side):
            g3[q, e].wait_recv()
        for half in range(2):
            at = slice(half * width + done, half * width + done + gbuf.shape[-1])
            for s in range(side):
                for f in range(side):
                    px, py = (f, s) if half == 0 else (s, f)
                    a = 2 * (px * side + py)
                    b = 2 * (side * side + py * side + px)
                    out_ref[a:a + 2, at] = gbuf[half, s, f, 0:2]
                    out_ref[b:b + 2, at] = gbuf[half, s, f, 2:4]
        done += gbuf.shape[-1]

    for group in (in1, in2, in3, g1, g2, g3):
        for copy in group.values():
            copy.wait_send()
    swap.wait_send()


def combine(part, tokens, w_o, side):
    seq_count, dim = tokens.shape
    steps, part_rows, head_dim = part.shape
    seqs = seq_count // steps
    q_heads = part_rows // seqs - 2
    parts = part.reshape(2, side, part_rows, head_dim)
    width = dim // 2
    near = width * 3 // 5 // 512 * 512
    depth = w_o.shape[0]
    dma = pltpu.SemaphoreType.DMA
    hbm = pl.BlockSpec(memory_space=pl.ANY)
    piece = (side, part_rows, head_dim)
    small = (side, 2 * q_heads + 2 * seqs, head_dim)
    return pl.pallas_call(
        functools.partial(combine_body, side, q_heads, seqs),
        out_shape=jax.ShapeDtypeStruct(tokens.shape, F32),
        in_specs=[pl.BlockSpec(memory_space=pltpu.VMEM), hbm],
        out_specs=pl.BlockSpec(memory_space=pltpu.VMEM),
        scratch_shapes=[
            pltpu.VMEM(piece, F32), pltpu.VMEM(piece, F32), pltpu.VMEM(piece, F32),
            pltpu.VMEM(small, F32), pltpu.VMEM(small, F32),
            pltpu.VMEM((side + 1, seqs, head_dim), F32),
            pltpu.VMEM((4 * q_heads, head_dim), F32),
            pltpu.VMEM((8, depth), F32),
            pltpu.VMEM((depth, width), BF16),
            pltpu.VMEM((2, side, side, 4, near), F32),
            pltpu.VMEM((2, side, side, 4, width - near), F32),
            dma((4,)),
            dma((side,)), dma((side,)),
            dma((side,)), dma((side,)),
            dma((side,)), dma((side,)),
            dma, dma,
            dma((2, side)), dma((2, side)),
            dma((2, side, side)), dma((2, side, side)),
            dma((2, side)), dma((2, side)),
        ],
        compiler_params=pltpu.CompilerParams(collective_id=1, has_side_effects=True, vmem_limit_bytes=LIMIT_C),
        name="combine",
    )(parts, w_o)


def solution(mesh):
    cache_spec = P('dp', 'sp', None, None)
    side = int(round((mesh.shape['sp'] // 2) ** 0.5))

    def device_step(tokens, positions, k_cache, v_cache, w_q, w_k, w_v, w_o, attn_norm, q_norm, k_norm):
        seq_count, slots, kv_heads, head_dim = k_cache.shape
        shard_start = (lax.axis_index('sp') * slots).astype(jnp.int32).reshape(1)
        seqs = 8
        heads = project(seqs, tokens, positions, w_q, w_k, w_v, attn_norm, q_norm, k_norm)
        k_upd, v_upd, part, new_kv = attention(seqs, heads, positions, shard_start, k_cache, v_cache)
        mixed = combine(part, tokens, w_o, side)
        block_out = (tokens.astype(F32) + mixed).astype(BF16)
        return block_out, k_upd, v_upd, new_kv

    return jax.shard_map(device_step, mesh=mesh, in_specs=(P('dp', None), P('dp'), cache_spec, cache_spec, P(), P(), P(), P(), P(), P(), P()), out_specs=(P('dp', None), cache_spec, cache_spec, P('dp', None, None, None)), check_vma=False)
```

```python
import functools

import jax
import jax.numpy as jnp
import numpy as np
from jax import lax
from jax.experimental import pallas as pl
from jax.experimental.pallas import tpu as pltpu
from jax.sharding import PartitionSpec as P

NORM_EPS = 1e-6
ROPE_THETA = 1000000.0
NEG_FILL = -1e30
MESH = pl.DeviceIdType.MESH
F32 = jnp.float32
BF16 = jnp.bfloat16
MIB = 1024 * 1024
LIMIT_A = 27 * MIB
LIMIT_B = 28 * MIB
LIMIT_C = 37 * MIB


def project_body(seq_count, q_heads, kv_heads, head_dim, tok_ref, gain_ref, qn_ref, kn_ref, pos_ref, freq_ref, wq_ref, wk_ref, wv_ref,
                 heads, tok, hid, wbuf, w_sem, t_sem, s_sem, r_sem):
    me = lax.axis_index("sp")
    core = lax.rem(me, 2)
    partner = me + 1 - 2 * core
    dim = tok_ref.shape[1]
    slots, _, width = wbuf.shape
    chunks = w_sem.shape[0]
    per = width // head_dim
    splits = w_sem.shape[1]
    rows = dim // splits
    kv_chunks = kv_heads // 2 // per

    def first_head(i, side):
        if i < kv_chunks:
            return side * (kv_heads // 2) + i * per, wk_ref, side * (kv_heads // 2) + i * per
        if i < 2 * kv_chunks:
            own = side * (kv_heads // 2) + (i - kv_chunks) * per
            return kv_heads + own, wv_ref, own
        own = side * (q_heads // 2) + (i - 2 * kv_chunks) * per
        return 2 * kv_heads + own, wq_ref, own

    sequence = list(range(2 * kv_chunks, chunks)) + list(range(2 * kv_chunks))

    def fetch(n, j):
        _, ref, head = first_head(sequence[n], core)
        return pltpu.make_async_copy(
            ref.at[pl.ds(j * rows, rows), pl.ds(pl.multiple_of(head * head_dim, 128), width)],
            wbuf.at[n % slots, pl.ds(j * rows, rows), :], w_sem.at[n, j])

    load = pltpu.make_async_copy(tok_ref, tok, t_sem)
    load.start()
    pieces = [(i, j) for i in range(chunks) for j in range(splits)]
    ahead = 5
    for i, j in pieces[:ahead]:
        fetch(i, j).start()

    barrier = pltpu.get_barrier_semaphore()
    pl.semaphore_signal(barrier, inc=1, device_id={"sp": partner}, device_id_type=MESH)

    eye = lax.broadcasted_iota(jnp.int32, (seq_count, seq_count), 0) == lax.broadcasted_iota(jnp.int32, (seq_count, seq_count), 1)
    pos = jnp.sum(jnp.where(eye, pos_ref[...].astype(F32), 0.0), axis=1, keepdims=True)
    angles = pos * freq_ref[...]
    cos = jnp.cos(angles)
    lower = lax.broadcasted_iota(jnp.int32, (seq_count, head_dim), 1) < head_dim // 2
    sin = jnp.sin(angles)
    sin = jnp.where(lower, -sin, sin)
    q_gain = qn_ref[...].astype(F32)
    k_gain = kn_ref[...].astype(F32)
    load.wait()
    values = tok[...].astype(F32)
    scale = lax.rsqrt(jnp.mean(values * values, axis=-1, keepdims=True) + NORM_EPS)
    for j in range(dim // 128):
        at = slice(j * 128, (j + 1) * 128)
        hid[:, at] = (tok[:, at].astype(F32) * scale * gain_ref[j:j + 1, :].astype(F32)).astype(BF16)
    pl.semaphore_wait(barrier, 1)

    swaps = []
    blocks, _, block, _ = heads.shape
    for turn, i in enumerate(sequence):
        acc = None
        for j in range(splits):
            at = turn * splits + j
            fetch(turn, j).wait()
            if at + ahead < len(pieces):
                fetch(*pieces[at + ahead]).start()
            part = jnp.dot(hid[:, j * rows:(j + 1) * rows], wbuf[turn % slots, j * rows:(j + 1) * rows, :], preferred_element_type=F32)
            acc = part if acc is None else acc + part
        acc = acc.astype(BF16).astype(F32)
        at = first_head(i, core)[0]
        for n in range(per):
            value = acc[:, n * head_dim:(n + 1) * head_dim]
            if not kv_chunks <= i < 2 * kv_chunks:
                scale = lax.rsqrt(jnp.mean(value * value, axis=-1, keepdims=True) + NORM_EPS)
                value = value * scale * (k_gain if i < kv_chunks else q_gain)
                value = value * cos + pltpu.roll(value, head_dim // 2, 1) * sin
                value = value.astype(BF16).astype(F32)
            for m in range(blocks):
                heads[m, at + n] = value[m * block:(m + 1) * block]
        span = heads.at[:, pl.ds(at, per)]
        copy = pltpu.make_async_remote_copy(
            src_ref=span, dst_ref=span, send_sem=s_sem.at[i], recv_sem=r_sem.at[i],
            device_id={"sp": partner}, device_id_type=MESH)
        copy.start()
        swaps.append(copy)
    for copy in swaps:
        copy.wait()


def project(seqs, tokens, positions, w_q, w_k, w_v, attn_norm, q_norm, k_norm):
    seq_count, dim = tokens.shape
    head_dim = q_norm.shape[0]
    q_heads = w_q.shape[1] // head_dim
    kv_heads = w_k.shape[1] // head_dim
    width = 4 * head_dim
    chunks = (w_q.shape[1] + w_k.shape[1] + w_v.shape[1]) // 2 // width
    splits = 2
    half = ROPE_THETA ** (-np.arange(head_dim // 2, dtype=np.float64) * 2.0 / head_dim)
    freq = jnp.asarray(np.concatenate([half, half]).astype(np.float32)).reshape(1, head_dim)
    vmem = pl.BlockSpec(memory_space=pltpu.VMEM)
    hbm = pl.BlockSpec(memory_space=pl.ANY)
    dma = pltpu.SemaphoreType.DMA
    return pl.pallas_call(
        functools.partial(project_body, seq_count, q_heads, kv_heads, head_dim),
        out_shape=jax.ShapeDtypeStruct((seq_count // seqs, q_heads + 2 * kv_heads, seqs, head_dim), F32),
        in_specs=[hbm, vmem, vmem, vmem, vmem, vmem, hbm, hbm, hbm],
        out_specs=vmem,
        scratch_shapes=[
            pltpu.VMEM((seq_count, dim), BF16),
            pltpu.VMEM((seq_count, dim), BF16),
            pltpu.VMEM((4, dim, width), BF16),
            dma((chunks, splits)), dma, dma((chunks,)), dma((chunks,)),
        ],
        compiler_params=pltpu.CompilerParams(collective_id=0, has_side_effects=True, vmem_limit_bytes=LIMIT_A),
        name="project",
    )(*[pltpu.with_memory_space_constraint(a, pltpu.HBM) for a in (
        tokens, attn_norm.reshape(-1, 128), q_norm.reshape(1, -1), k_norm.reshape(1, -1), positions.reshape(1, -1), freq, w_q, w_k, w_v)])


def attn_body(steps, seqs, slots, kv_heads, q_heads, pos_ref, start_ref, heads, k_ref, v_ref, ko_ref, vo_ref, obuf, nk_ref,
              kbuf0, kbuf1, kbuf2, vbuf0, vbuf1, vbuf2, nkbuf, sc_ref, pw_ref, o_sem):
    head_dim = k_ref.shape[-1]
    scale = head_dim ** -0.5
    cols = slots * kv_heads
    group = q_heads // kv_heads
    o_rows = seqs * q_heads
    kbufs, vbufs = (kbuf0, kbuf1, kbuf2), (vbuf0, vbuf1, vbuf2)

    def span(i):
        return pl.ds(i * seqs, seqs)

    def caches_out(i):
        return [
            pltpu.make_async_copy(kbufs[i % 3], ko_ref.at[span(i)], o_sem.at[i, 2]),
            pltpu.make_async_copy(vbufs[i % 3], vo_ref.at[span(i)], o_sem.at[i, 3]),
        ]

    def rest_out(i):
        return [
            pltpu.make_async_copy(nkbuf.at[span(i)], nk_ref.at[span(i)], o_sem.at[i, 1]),
        ]

    row_id = lax.broadcasted_iota(jnp.int32, (q_heads, cols), 0)
    col_id = lax.broadcasted_iota(jnp.int32, (q_heads, cols), 1)
    own_head = jnp.zeros((q_heads, cols), jnp.int32)
    for h in range(1, kv_heads):
        own_head += (row_id >= h * group).astype(jnp.int32)
    slot_of = jnp.where(lax.rem(col_id, kv_heads) == own_head, lax.div(col_id, kv_heads), 1 << 20)
    upper = lax.broadcasted_iota(jnp.int32, (2 * kv_heads, head_dim), 0) >= kv_heads
    diag_r = lax.broadcasted_iota(jnp.int32, (q_heads, head_dim), 0)
    diag_c = lax.broadcasted_iota(jnp.int32, (q_heads, head_dim), 1)
    diag = diag_r == diag_c

    def bring(i, b):
        kbufs[i % 3][b] = k_ref[i * seqs + b]
        vbufs[i % 3][b] = v_ref[i * seqs + b]

    for b in range(seqs):
        bring(0, b)
    for i in range(steps):
        kbuf, vbuf = kbufs[i % 3], vbufs[i % 3]
        rows_of = heads.at[i].reshape((2 * kv_heads + q_heads) * seqs, head_dim)
        if i >= 2:
            for copy in caches_out(i - 2):
                copy.wait()
        for b in range(seqs):
            rel = pos_ref[i * seqs + b] - start_ref[0]
            at = i * seqs + b
            k_new = rows_of[pl.ds(b, kv_heads, stride=seqs), :]
            v_new = rows_of[pl.ds(b + kv_heads * seqs, kv_heads, stride=seqs), :]
            nkbuf[at] = jnp.concatenate([k_new, v_new], axis=0).astype(BF16)

            @pl.when((rel >= 0) & (rel < slots))
            def _(b=b, rel=rel, k_new=k_new, v_new=v_new, kbuf=kbuf, vbuf=vbuf):
                tile = lax.div(rel, 2)
                hit = upper == (lax.rem(rel, 2) == 1)
                k_two = jnp.concatenate([k_new, k_new], axis=0)
                v_two = jnp.concatenate([v_new, v_new], axis=0)
                kbuf[b, tile] = jnp.where(hit, k_two, kbuf[b, tile].astype(F32)).astype(BF16)
                vbuf[b, tile] = jnp.where(hit, v_two, vbuf[b, tile].astype(F32)).astype(BF16)
        for copy in caches_out(i):
            copy.start()
        peaks = []
        for b in range(seqs):
            rel = pos_ref[i * seqs + b] - start_ref[0]
            keys = kbuf[b].reshape(cols, head_dim)
            query = rows_of[pl.ds(b + 2 * kv_heads * seqs, q_heads, stride=seqs), :].astype(BF16)
            scores = lax.dot_general(query, keys, (((1,), (1,)), ((), ())), preferred_element_type=F32) * scale
            scores = jnp.where(slot_of <= rel, scores, -jnp.inf)
            sc_ref[b] = scores
            if i + 1 < steps:
                bring(i + 1, b)
            peaks.append(jnp.max(scores, axis=1, keepdims=True))
        totals = []
        for b in range(seqs):
            rel = pos_ref[i * seqs + b] - start_ref[0]
            shift = jnp.where(rel < 0, 0.0, peaks[b])
            weights = jnp.exp(sc_ref[b] - shift)
            totals.append(jnp.sum(weights, axis=1, keepdims=True))
            pw_ref[b] = weights.astype(BF16)
        for b in range(seqs):
            vals = vbuf[b].reshape(cols, head_dim)
            obuf[i, pl.ds(b * q_heads, q_heads), :] = jnp.dot(pw_ref[b], vals, preferred_element_type=F32)
            peak = jnp.maximum(peaks[b], NEG_FILL)
            obuf[i, pl.ds(o_rows + b, 1), :] = jnp.sum(jnp.where(diag, peak, 0.0), axis=0, keepdims=True)
            obuf[i, pl.ds(o_rows + seqs + b, 1), :] = jnp.sum(jnp.where(diag, totals[b], 0.0), axis=0, keepdims=True)
        for copy in rest_out(i):
            copy.start()

    for i in range(steps):
        for copy in rest_out(i) + (caches_out(i) if i >= steps - 2 else []):
            copy.wait()


def attention(seqs, heads, positions, shard_start, k_cache, v_cache):
    seq_count, slots, kv_heads, head_dim = k_cache.shape
    q_heads = heads.shape[1] - 2 * kv_heads
    steps = seq_count // seqs
    pairs = slots // 2
    part_rows = seqs * q_heads + 2 * seqs
    k4 = k_cache.reshape(seq_count, pairs, 2 * kv_heads, head_dim)
    v4 = v_cache.reshape(seq_count, pairs, 2 * kv_heads, head_dim)
    hbm = pl.BlockSpec(memory_space=pl.ANY)
    vmem = pl.BlockSpec(memory_space=pltpu.VMEM)
    smem = pl.BlockSpec(memory_space=pltpu.SMEM)
    dma = pltpu.SemaphoreType.DMA
    k_out, v_out, part, new_kv = pl.pallas_call(
        functools.partial(attn_body, steps, seqs, slots, kv_heads, q_heads),
        in_specs=[smem, smem, vmem, vmem, vmem],
        out_specs=[hbm, hbm, vmem, hbm],
        out_shape=[
            jax.ShapeDtypeStruct(k4.shape, BF16),
            jax.ShapeDtypeStruct(v4.shape, BF16),
            jax.ShapeDtypeStruct((steps, part_rows, head_dim), F32),
            jax.ShapeDtypeStruct((seq_count, 2 * kv_heads, head_dim), BF16),
        ],
        scratch_shapes=[
            *[pltpu.VMEM((seqs,) + k4.shape[1:], BF16)] * 6,
            pltpu.VMEM((seq_count, 2 * kv_heads, head_dim), BF16),
            pltpu.VMEM((seqs, q_heads, slots * kv_heads), F32),
            pltpu.VMEM((seqs, q_heads, slots * kv_heads), BF16),
            dma((steps, 4)),
        ],
        compiler_params=pltpu.CompilerParams(vmem_limit_bytes=LIMIT_B),
        name="attend",
    )(positions, shard_start, heads, k4, v4)
    return (k_out.reshape(k_cache.shape), v_out.reshape(v_cache.shape), part,
            new_kv.reshape(seq_count, 2, kv_heads, head_dim))


def blend(stats):
    peak = stats[0][0]
    for m, _ in stats[1:]:
        peak = jnp.maximum(peak, m)
    factors = [jnp.exp(m - peak) for m, _ in stats]
    total = factors[0] * stats[0][1]
    for f, (_, l) in zip(factors[1:], stats[1:]):
        total += f * l
    return peak, total, factors


def combine_body(side, q_heads, seqs, o_ref, wo_ref, out_ref, r1, s1, r2, s2, r3, fin, obuf, lhs, wbuf, gbuf0, gbuf1,
                 w_sem, a_s, a_r, b_s, b_r, c_s, c_r, d_s, d_r, e_s, e_r, f_s, f_r, h_s, h_r):
    me = lax.axis_index("sp")
    core = lax.rem(me, 2)
    chip = lax.div(me, 2)
    x = lax.rem(chip, side)
    y = lax.div(chip, side)
    first = x * (1 - core) + y * core
    second = y * (1 - core) + x * core
    stride1 = 2 * (1 - core) + 2 * side * core
    stride2 = 2 * side * (1 - core) + 2 * core
    partner = me + 1 - 2 * core
    head_dim = o_ref.shape[-1]
    gbufs = (gbuf0, gbuf1)
    depth, width = wbuf.shape
    w_parts = w_sem.shape[0]
    w_rows = depth // w_parts
    rows = 2 * q_heads
    body = side * rows
    stat_m, stat_l = pl.ds(body, seqs), pl.ds(body + seqs, seqs)
    order = [side // 2] + [d for d in range(1, side) if d != side // 2]

    def peer1(d):
        return me + (lax.rem(first + d, side) - first) * stride1

    def peer2(d):
        return me + (lax.rem(second + d, side) - second) * stride2

    def send(src, dst, ssem, rsem, to):
        copy = pltpu.make_async_remote_copy(src_ref=src, dst_ref=dst, send_sem=ssem, recv_sem=rsem, device_id={"sp": to}, device_id_type=MESH)
        copy.start()
        return copy

    barrier = pltpu.get_barrier_semaphore()
    neighbours = [partner] + [peer1(d) for d in range(1, side)] + [peer2(d) for d in range(1, side)]
    for n in neighbours:
        pl.semaphore_signal(barrier, inc=1, device_id={"sp": n}, device_id_type=MESH)
    pl.semaphore_wait(barrier, len(neighbours))

    in1 = {}
    for d in order + [0]:
        in1[d] = send(o_ref.at[1 - core, lax.rem(second + d, side)], r1.at[d], a_s.at[d], a_r.at[d], partner)
    w_copies = []
    for i in range(w_parts):
        copy = pltpu.make_async_copy(
            wo_ref.at[pl.ds(i * w_rows, w_rows), pl.ds(pl.multiple_of(core * width, 128), width)],
            wbuf.at[pl.ds(i * w_rows, w_rows), :], w_sem.at[i])
        copy.start()
        w_copies.append(copy)
    in2 = {}
    for d in order + [0]:
        in1[d].wait_recv()
        piece = lax.rem(first + d, side)
        peak, total, fac = blend([(o_ref[core, piece, stat_m, :], o_ref[core, piece, stat_l, :]), (r1[d, stat_m, :], r1[d, stat_l, :])])
        s1[d, stat_m, :] = peak
        s1[d, stat_l, :] = total
        cols = [jnp.transpose(f) for f in fac]
        for seq in range(seqs):
            at = pl.ds(seq * q_heads, q_heads)
            s1[d, at, :] = (o_ref[core, piece, at, :] * cols[0][:q_heads, seq:seq + 1]
                            + r1[d, at, :] * cols[1][:q_heads, seq:seq + 1])
        if d:
            in2[d] = send(s1.at[d], r2.at[d], b_s.at[d], b_r.at[d], peer1(d))
    for d in order:
        in2[d].wait_recv()
    peak, total, fac = blend([(s1[0, stat_m, :], s1[0, stat_l, :])] + [(r2[d, stat_m, :], r2[d, stat_l, :]) for d in range(1, side)])
    cols = [jnp.transpose(f) for f in fac]
    for k in range(side):
        for i in range(2):
            seq = 2 * k + i
            at = pl.ds(seq * q_heads, q_heads)
            value = s1[0, at, :] * cols[0][:q_heads, seq:seq + 1]
            for d in range(1, side):
                value += r2[d, at, :] * cols[d][:q_heads, seq:seq + 1]
            s2[k, pl.ds(i * q_heads, q_heads), :] = value
        s2[k, pl.ds(rows, seqs), :] = peak
        s2[k, pl.ds(rows + seqs, seqs), :] = total
    in3 = {}
    for d in order:
        in3[d] = send(s2.at[lax.rem(second + d, side)], r3.at[d], c_s.at[d], c_r.at[d], peer2(d))
    for d in order:
        in3[d].wait_recv()
    low, high = pl.ds(rows, seqs), pl.ds(rows + seqs, seqs)
    peak, total, fac = blend([(s2[0, low, :], s2[0, high, :])] + [(r3[d, low, :], r3[d, high, :]) for d in range(1, side)])
    for n, tile in enumerate(fac + [total]):
        fin[n] = tile
    mine = pl.ds(2 * second, 2)
    cols = [jnp.transpose(jnp.concatenate([fin[n, mine, :]] * (seqs // 2), axis=0)) for n in range(side + 1)]
    for i in range(2):
        at = pl.ds(i * q_heads, q_heads)
        value = s2[second, at, :] * cols[0][:q_heads, i:i + 1]
        for d in range(1, side):
            value += r3[d, at, :] * cols[d][:q_heads, i:i + 1]
        value = value / cols[side][:q_heads, i:i + 1]
        obuf[pl.ds(pl.multiple_of(core * rows, 8) + i * q_heads, q_heads), :] = value.astype(BF16).astype(F32)
    own = obuf.at[pl.ds(pl.multiple_of(core * rows, 8), rows)]
    swap = send(own, own, d_s, d_r, partner)
    lhs[...] = jnp.zeros_like(lhs)
    for copy in w_copies:
        copy.wait()
    swap.wait_recv()
    for h in range(q_heads):
        lhs[0:4, h * head_dim:(h + 1) * head_dim] = obuf[pl.ds(h, 4, stride=q_heads), :]
    left = lhs[...].astype(BF16)
    g1, g2, g3 = {}, {}, {}
    n_step = 512
    done = 0
    for q, gbuf in enumerate(gbufs):
        own = gbuf.at[core, second, first]
        for n in range(0, gbuf.shape[-1], n_step):
            gbuf[core, second, first, :, n:n + n_step] = jnp.dot(left, wbuf[:, done + n:done + n + n_step], preferred_element_type=F32)[0:4]
        done += gbuf.shape[-1]
        for d in order:
            g1[q, d] = send(own, own, e_s.at[q, d], e_r.at[q, d], peer1(d))
        for e in order:
            g2[q, e, 0] = send(own, own, f_s.at[q, e, 0], f_r.at[q, e, 0], peer2(e))
    for q, gbuf in enumerate(gbufs):
        for d in order[1:] + order[:1]:
            f_from = lax.rem(first - d + side, side)
            got = gbuf.at[core, second, f_from]
            g1[q, d].wait_recv()
            for e in order:
                g2[q, e, d] = send(got, got, f_s.at[q, e, d], f_r.at[q, e, d], peer2(e))
        row = gbuf.at[core, second]
        g3[q, 0] = send(row, row, h_s.at[q, 0], h_r.at[q, 0], partner)
    for q, gbuf in enumerate(gbufs):
        for e in order[1:] + order[:1]:
            row = gbuf.at[core, lax.rem(second - e + side, side)]
            for d in range(side):
                g2[q, e, d].wait_recv()
            g3[q, e] = send(row, row, h_s.at[q, e], h_r.at[q, e], partner)
    done = 0
    for q, gbuf in enumerate(gbufs):
        for e in range(side):
            g3[q, e].wait_recv()
        for half in range(2):
            at = slice(half * width + done, half * width + done + gbuf.shape[-1])
            for s in range(side):
                for f in range(side):
                    px, py = (f, s) if half == 0 else (s, f)
                    a = 2 * (px * side + py)
                    b = 2 * (side * side + py * side + px)
                    out_ref[a:a + 2, at] = gbuf[half, s, f, 0:2]
                    out_ref[b:b + 2, at] = gbuf[half, s, f, 2:4]
        done += gbuf.shape[-1]

    for group in (in1, in2, in3, g1, g2, g3):
        for copy in group.values():
            copy.wait_send()
    swap.wait_send()


def combine(part, tokens, w_o, side):
    seq_count, dim = tokens.shape
    steps, part_rows, head_dim = part.shape
    seqs = seq_count // steps
    q_heads = part_rows // seqs - 2
    parts = part.reshape(2, side, part_rows, head_dim)
    width = dim // 2
    near = width * 3 // 5 // 512 * 512
    depth = w_o.shape[0]
    dma = pltpu.SemaphoreType.DMA
    hbm = pl.BlockSpec(memory_space=pl.ANY)
    piece = (side, part_rows, head_dim)
    small = (side, 2 * q_heads + 2 * seqs, head_dim)
    return pl.pallas_call(
        functools.partial(combine_body, side, q_heads, seqs),
        out_shape=jax.ShapeDtypeStruct(tokens.shape, F32),
        in_specs=[pl.BlockSpec(memory_space=pltpu.VMEM), hbm],
        out_specs=pl.BlockSpec(memory_space=pltpu.VMEM),
        scratch_shapes=[
            pltpu.VMEM(piece, F32), pltpu.VMEM(piece, F32), pltpu.VMEM(piece, F32),
            pltpu.VMEM(small, F32), pltpu.VMEM(small, F32),
            pltpu.VMEM((side + 1, seqs, head_dim), F32),
            pltpu.VMEM((4 * q_heads, head_dim), F32),
            pltpu.VMEM((8, depth), F32),
            pltpu.VMEM((depth, width), BF16),
            pltpu.VMEM((2, side, side, 4, near), F32),
            pltpu.VMEM((2, side, side, 4, width - near), F32),
            dma((4,)),
            dma((side,)), dma((side,)),
            dma((side,)), dma((side,)),
            dma((side,)), dma((side,)),
            dma, dma,
            dma((2, side)), dma((2, side)),
            dma((2, side, side)), dma((2, side, side)),
            dma((2, side)), dma((2, side)),
        ],
        compiler_params=pltpu.CompilerParams(collective_id=1, has_side_effects=True, vmem_limit_bytes=LIMIT_C),
        name="combine",
    )(parts, w_o)


def solution(mesh):
    cache_spec = P('dp', 'sp', None, None)
    side = int(round((mesh.shape['sp'] // 2) ** 0.5))

    def device_step(tokens, positions, k_cache, v_cache, w_q, w_k, w_v, w_o, attn_norm, q_norm, k_norm):
        seq_count, slots, kv_heads, head_dim = k_cache.shape
        shard_start = (lax.axis_index('sp') * slots).astype(jnp.int32).reshape(1)
        seqs = 8
        heads = project(seqs, tokens, positions, w_q, w_k, w_v, attn_norm, q_norm, k_norm)
        k_upd, v_upd, part, new_kv = attention(seqs, heads, positions, shard_start, k_cache, v_cache)
        mixed = combine(part, tokens, w_o, side)
        block_out = (tokens.astype(F32) + mixed).astype(BF16)
        return block_out, k_upd, v_upd, new_kv

    return jax.shard_map(device_step, mesh=mesh, in_specs=(P('dp', None), P('dp'), cache_spec, cache_spec, P(), P(), P(), P(), P(), P(), P()), out_specs=(P('dp', None), cache_spec, cache_spec, P('dp', None, None, None)), check_vma=False)
```
